256 devices in a mesh: seq: 64 (over x, z, core), head: 4 (over y).
Axes of the slice: x: 4, y: 4, z: 8, core: 2. Of those that a mesh axis runs over, the one named last changes fastest.
Arguments:
- queries: bfloat16 [32768, 1024], P('seq', 'head'), may hold values from -6 to 6
- key_vectors: bfloat16 [32768, 1024], P('seq', 'head'), may hold values from -6 to 6
- values: bfloat16 [32768, 2048], P('seq', 'head'), may hold values from -6 to 6
- log_gate: bfloat16 [32768, 1024], P('seq', 'head'), may hold values from -1.6 to 0, as said below
- out_gate: bfloat16 [32768, 2048], P('seq', 'head'), may hold values from -6 to 6
- norm_gain: float32 [2048], P('head'), may hold values from 0.5 to 1.5
- out_weight: bfloat16 [2048, 2048], P('head'), may hold values from -0.1875 to 0.1875
Outputs:
- mixed: bfloat16 [32768, 2048], P('seq', 'head')
The draws below stay inside these ranges and needn't reach their ends.
Inputs may be any that keep to these rules, and one draw needn't show every extreme that they name: `log_gate`: every entry is below zero.
All inputs are finite; a program needn't handle non-finite values.
Results may differ from the reference program's by a relative error of at most 0.017.
Values may be sent and summed in bfloat16 or wider, within the bound.
A program may use at most 128 MiB of HBM per device.

```python
import jax
import jax.numpy as jnp
from jax import lax

D = 2048
H = 4
DK = 256
DV = 512
SPAN = 64
TOK_DEV = 512
SEQUENCE_TOKENS = 32768
N_HEAD = 4


def draw_log_gate(key, part):
    parallel_lanes = jax.random.split(key, 7)
    blocks_all = SEQUENCE_TOKENS // TOK_DEV
    quick_count = H // 2
    order = jax.random.permutation(parallel_lanes[0], H)
    quick_head = order < quick_count
    quick_rate = jnp.exp(jax.random.uniform(parallel_lanes[1], (H, DK), minval=jnp.log(0.02), maxval=jnp.log(0.06)))
    slow_rate = jnp.exp(jax.random.uniform(parallel_lanes[2], (H, DK), minval=jnp.log(0.05), maxval=jnp.log(0.25))) / SEQUENCE_TOKENS
    base_rate = jnp.where(quick_head[:, None], quick_rate, slow_rate).reshape(1, 1, H * DK)
    device_factor = jnp.exp(jax.random.uniform(parallel_lanes[3], (blocks_all, 1, H * DK), minval=jnp.log(0.5), maxval=jnp.log(2.0)))
    roughness = jax.random.uniform(parallel_lanes[4], (blocks_all, TOK_DEV, H * DK), minval=0.5, maxval=1.5)
    decay_factor = (base_rate * device_factor * roughness).reshape(SEQUENCE_TOKENS, H * DK)
    block_offset = jax.random.randint(parallel_lanes[5], (2,), 0, SEQUENCE_TOKENS)
    block_length = jnp.log(jax.random.uniform(parallel_lanes[6], (2,), minval=0.5, maxval=0.8))
    token_position = lax.iota(jnp.int32, SEQUENCE_TOKENS)
    token_block = jnp.sum(jnp.where(token_position[:, None] == block_offset[None, :], block_length[None, :], 0.0), axis=1)
    return (token_block[:, None] - decay_factor).astype(jnp.bfloat16)


def raised(entries, rng, source, target, parts, factor):
    def block_of(dim):
        return (jnp.arange(entries.shape[dim]) // (entries.shape[dim] // parts)).reshape((-1,) + (1,) * (entries.ndim - 1 - dim))

    near = jax.random.permutation(rng, parts)[block_of(target)]
    other_side = (block_of(target) + parts // 2) % parts
    return jnp.where((block_of(source) == near) | (block_of(source) == other_side), factor * entries, entries)


def steps_of(stream_key, dims, pieces, least, largest):
    def one(axis_at, shards_of):
        heights = jax.random.uniform(jax.random.fold_in(jax.random.fold_in(stream_key, 6), axis_at), (shards_of,), jnp.float32, least / len(pieces), largest / len(pieces))
        return jnp.repeat(jnp.exp(heights), dims[axis_at] // shards_of).reshape((-1,) + (1,) * (len(dims) - axis_at - 1))

    factor_of = one(*pieces[0])
    for cut in pieces[1:]:
        factor_of = factor_of * one(*cut)
    return factor_of


def normal_values(stream_key, shape, scale, most, cuts=(), kind=jnp.bfloat16):
    factor_of = steps_of(stream_key, shape, cuts, -0.22, 0.18) if cuts else 1.0
    result = jax.random.normal(stream_key, shape, jnp.float32) * scale * factor_of
    return jnp.minimum(jnp.maximum(result, -most), most).astype(kind)


def noise_with(own_key, dims, scale, reach, cuts, heavy, dtype=jnp.bfloat16):
    array = scale * jax.random.normal(own_key, dims, jnp.float32)
    if cuts:
        array = array * steps_of(own_key, dims, cuts, -0.22, 0.18)
    return jnp.clip(raised(array, jax.random.fold_in(own_key, 3), *heavy), -reach, reach).astype(dtype)


def setup_inputs(seed: int = 0) -> dict:
    streams_of = jax.random.split(jax.random.key(seed), 8)
    queries = normal_values(streams_of[0], (SEQUENCE_TOKENS, H * DK), 1.0, 6.0, ((0, 64), (1, 4)))
    key_vectors = normal_values(streams_of[1], (SEQUENCE_TOKENS, H * DK), 1.0, 6.0, ((0, 64), (1, 4)))
    values = normal_values(streams_of[2], (SEQUENCE_TOKENS, H * DV), 1.0, 6.0, ((0, 64), (1, 4)))
    log_gate = draw_log_gate(jax.random.fold_in(streams_of[7], 71), 0)
    out_gate = normal_values(streams_of[4], (SEQUENCE_TOKENS, H * DV), 1.0, 6.0, ((0, 64), (1, 4)))
    norm_gain = jnp.clip(1.0 + 0.1 * jax.random.normal(streams_of[5], (H * DV,), jnp.float32), 0.5, 1.5)
    out_weight = noise_with(streams_of[6], (H * DV, D), (H * DV) ** -0.5, 0.1875, ((0, 4),), (0, 1, 4, 2.0))
    return {"queries": queries, "key_vectors": key_vectors, "values": values, "log_gate": log_gate, "out_gate": out_gate, "norm_gain": norm_gain, "out_weight": out_weight}


def lowered(array_in):
    return lax.optimization_barrier(array_in.astype(jnp.bfloat16)).astype(jnp.float32)

def reference(queries, key_vectors, values, log_gate, out_gate, norm_gain, out_weight):
    blocks = SEQUENCE_TOKENS // SPAN
    middle_pos = SPAN // 2
    causal = lax.iota(jnp.int32, SPAN)[:, None] >= lax.iota(jnp.int32, SPAN)[None, :]
    gain_table = norm_gain.reshape(H, DV)

    def advance(carried, block_in):
        query_b, key_b, value_b, gate_b, outer_b = block_in
        running = jnp.cumsum(gate_b.astype(jnp.float32), axis=0)
        middle = running[middle_pos:middle_pos + 1]
        ending = running[SPAN - 1:SPAN]
        query_f = query_b.astype(jnp.float32)
        key_f = key_b.astype(jnp.float32)
        value_f = value_b.astype(jnp.float32)
        q_inter = lowered(query_f * jnp.exp(running))
        q_intra = lowered(query_f * jnp.exp(running - middle))
        k_intra = lowered(key_f * jnp.exp(middle - running))
        k_state = lowered(key_f * jnp.exp(ending - running))
        scores = jnp.einsum('thd,shd->hts', q_intra, k_intra)
        weights = lowered(jnp.where(causal[None], scores, 0.0))
        local_part = jnp.einsum('hts,she->the', weights, value_f)
        carried_low = lowered(carried)
        carried_part = jnp.einsum('thd,hed->the', q_inter, carried_low)
        attention = local_part + carried_part
        spread = lax.optimization_barrier(jnp.mean(attention * attention, axis=-1, keepdims=True))
        normed = attention / jnp.sqrt(spread + 1e-05) * gain_table
        gated_out = (normed * jax.nn.silu(outer_b.astype(jnp.float32))).astype(jnp.bfloat16)
        block_state = jnp.einsum('the,thd->hed', value_f, k_state)
        carried = carried * jnp.exp(ending[0])[:, None, :] + block_state
        return (carried, gated_out.reshape(SPAN, H * DV))
    start_state = jnp.zeros((H, DV, DK), jnp.float32)
    inputs = (queries.reshape(blocks, SPAN, H, DK), key_vectors.reshape(blocks, SPAN, H, DK), values.reshape(blocks, SPAN, H, DV), log_gate.reshape(blocks, SPAN, H, DK), out_gate.reshape(blocks, SPAN, H, DV))
    unused_state, gated_all = lax.scan(advance, start_state, inputs)
    gated_all = gated_all.reshape(SEQUENCE_TOKENS, H * DV)
    group_width = H // N_HEAD * DV
    summed = jnp.zeros((SEQUENCE_TOKENS, D), jnp.float32)
    for group_index in range(N_HEAD):
        start_row = group_index * group_width
        end_row = start_row + group_width
        partial_value = jnp.dot(gated_all[:, start_row:end_row], out_weight[start_row:end_row], preferred_element_type=jnp.float32)
        summed = summed + lowered(partial_value)
    return summed.astype(jnp.bfloat16)
```

```python
import functools

import jax
import jax.numpy as jnp
from jax import lax
from jax.experimental import pallas as pl
from jax.experimental.pallas import tpu as pltpu
from jax.sharding import PartitionSpec as P

DK = 256
DV = 512
SPAN = 64
TOKENS = 64
ROWS = 16
LANES = 128
Z = 8
EARLY = 2
F32 = jnp.float32
BF16 = jnp.bfloat16
MESH = pl.DeviceIdType.MESH


def dot(a, b, dims=((1,), (0,))):
    return lax.dot_general(a, b, (dims, ((), ())), preferred_element_type=F32)


def kernel(
    n_seq, n_head,
    q_hbm, k_hbm, v_hbm, g_hbm, o_hbm, gain_hbm, w_hbm,
    out,
    q, k, v, g, o, gain, w, w_a, w_b,
    run, ends, kd, qg, att, act, state,
    log_out, log_in, half_out, half_in, own_half, decay,
    sum_out, sum_in, sums, spans,
    tile_out, tile_in, enter_out, enter_in, pass_out, carry,
    gated, mine, y_out, y_in,
    load_sem, w_sem, w_send, w_recv, hand_send, hand_recv,
    log_send, log_recv, half_send, half_recv, pass_send, pass_recv,
    sum_send, sum_recv, tile_send, tile_recv, enter_send, enter_recv,
    g_send, g_recv, y_send, y_recv,
):
    length = q.shape[0]
    blocks = length // SPAN
    pieces = length // TOKENS
    width = w_hbm.shape[1] // n_head
    half = DK // 2
    chips = n_seq // 2
    across = DV // LANES
    seq = lax.axis_index("seq")
    head = lax.axis_index("head")
    core = lax.rem(seq, 2)
    chip = lax.div(seq, 2)
    first = core == 0
    at_x = lax.div(chip, Z)
    at_z = lax.rem(chip, Z)
    head_a = head + 1 - 2 * lax.rem(head, 2)
    head_b = n_head - 1 - head
    head_c = n_head - 1 - head_a
    sibling = {"seq": seq + 1 - 2 * core, "head": head}
    near_a = {"seq": seq, "head": head_a}
    near_b = {"seq": seq, "head": head_b}
    steps = [
        (dx, (Z // 2 + (-dz // 2 if dz % 2 else dz // 2)) % Z)
        for dz in range(Z) for dx in (2, 1, 3, 0)
    ]
    others = [
        lax.rem(at_x + dx, chips // Z) * Z + lax.rem(at_z + dz, Z)
        for dx, dz in steps if dx or dz
    ]

    def mate(other):
        return {"seq": other * 2 + core, "head": head}

    def columns(which):
        return pl.ds(pl.multiple_of(which * width, 128), width)

    loads = [
        pltpu.make_async_copy(src, dst, load_sem.at[i])
        for i, (src, dst) in enumerate(
            ((g_hbm, g), (k_hbm, k), (v_hbm, v), (q_hbm, q), (o_hbm, o), (gain_hbm, gain))
        )
    ]
    for load in loads:
        load.start()
    w_loads = [
        pltpu.make_async_copy(w_hbm.at[:, columns(which)], w.at[j], w_sem.at[j])
        for j, which in enumerate((head, head_a, head_b))
    ]
    barrier = pltpu.get_barrier_semaphore()
    friends = [mate(other) for other in others] + [sibling, near_a, near_b]
    for friend in friends:
        pl.semaphore_signal(barrier, inc=1, device_id=friend, device_id_type=MESH)

    def remote(src, dst, send, recv, device):
        return pltpu.make_async_remote_copy(
            src_ref=src, dst_ref=dst, send_sem=send, recv_sem=recv,
            device_id=device, device_id_type=MESH,
        )

    tri = (
        lax.broadcasted_iota(jnp.int32, (SPAN, SPAN), 0)
        >= lax.broadcasted_iota(jnp.int32, (SPAN, SPAN), 1)
    )
    ones = jnp.where(tri, 1.0, 0.0).astype(BF16)
    loads[0].wait()
    total = jnp.zeros((1, DK), F32)
    endings = []
    for b in range(blocks):
        r = dot(ones, g[b * SPAN : (b + 1) * SPAN, :])
        run[b] = r
        endings.append(r[SPAN - 1 : SPAN, :])
        ends[b : b + 1, :] = total
        total = total + endings[b]
    log_out[...] = jnp.broadcast_to(total, log_out.shape)
    loads[1].wait()
    tail = jnp.zeros((1, DK), F32)
    for b in reversed(range(blocks)):
        part = slice(b * SPAN, (b + 1) * SPAN)
        kd[part, :] = (k[part, :].astype(F32) * jnp.exp((endings[b] - run[b]) + tail)).astype(BF16)
        tail = tail + endings[b]
    loads[2].wait()

    def half_state(which):
        cols = pl.ds(pl.multiple_of(which * half, 128), half)
        return dot(kd[:, cols], v[...], ((0,), (0,)))

    half_out[...] = half_state(1 - core).astype(BF16)
    own_half[...] = half_state(core)

    pl.semaphore_wait(barrier, len(friends))
    log_copy = remote(log_out, log_in, log_send.at[0], log_recv.at[0], sibling)
    log_copy.start()
    half_copy = remote(half_out, half_in, half_send.at[0], half_recv.at[0], sibling)
    half_copy.start()
    w_copies = [
        remote(
            w_hbm.at[:, columns(jnp.where(first, own, head_c))], dst.at[core],
            w_send.at[j], w_recv.at[j], device,
        )
        for j, (own, dst, device) in enumerate(((head_a, w_a, near_a), (head_b, w_b, near_b)))
    ]
    hand_copies = [
        remote(dst.at[core], dst.at[core], hand_send.at[j], hand_recv.at[j], sibling)
        for j, dst in enumerate((w_a, w_b))
    ]
    for load in loads[3:]:
        load.wait()
    state[...] = jnp.zeros_like(state)

    def column(row):
        lanes = jnp.broadcast_to(row, (128, DK)).T
        return jnp.concatenate([lanes] * across, axis=1)

    def local(b, _):
        part = pl.ds(pl.multiple_of(b * SPAN, SPAN), SPAN)
        r = run[b]
        middle = r[SPAN // 2 : SPAN // 2 + 1, :]
        ending = r[SPAN - 1 : SPAN, :]
        before = ends[pl.ds(b, 1), :]
        qf = q[part, :].astype(F32)
        kf = k[part, :].astype(F32)
        qi = qf * jnp.exp(r)
        qg[part, :] = (qi * jnp.exp(before)).astype(BF16)
        q_intra = (qf * jnp.exp(r - middle)).astype(BF16)
        k_intra = (kf * jnp.exp(middle - r)).astype(BF16)
        k_state = (kf * jnp.exp(ending - r)).astype(BF16)
        vb = v[part, :]
        scores = dot(q_intra, k_intra, ((1,), (1,)))
        weights = jnp.where(tri, scores, 0.0).astype(BF16)
        held = state[...]
        att[part, :] = dot(weights, vb) + dot(qi.astype(BF16), held.astype(BF16))
        state[...] = held * column(jnp.exp(ending)) + dot(k_state, vb, ((0,), (0,)))
        of = o[part, :].astype(F32)
        act[part, :] = of / (1.0 + jnp.exp(-of)) * gain[...]
        return 0

    log_copy.wait_recv()
    both = [jnp.where(first, row[:, :half], row[:, half:]) for row in (log_out[0:1, :], log_in[0:1, :])]
    sum_out[...] = both[0] + both[1]
    sum_copies = [
        remote(sum_out, sum_in.at[chip], sum_send.at[i], sum_recv.at[i], mate(other))
        for i, other in enumerate(others)
    ]
    for copy in sum_copies:
        copy.start()
    sum_in[chip] = sum_out[...]
    for i, row in enumerate(
        (jnp.where(first, both[0], both[1]), jnp.where(first, both[1], both[0]))
    ):
        decay[i] = jnp.broadcast_to(jnp.exp(row), (128, half)).T

    def decays(i, rows):
        return jnp.concatenate([decay[i, rows, :]] * across, axis=1)

    def halves(rows):
        own = own_half[rows, :]
        other = half_in[rows, :].astype(F32)
        return jnp.where(first, own, other), jnp.where(first, other, own)

    half_copy.wait_recv()
    for i in range(half // ROWS):
        rows = slice(i * ROWS, (i + 1) * ROWS)
        s0, s1 = halves(rows)
        chip_state = (decays(1, rows) * s0 + s1).astype(BF16)
        for j in range(across):
            tile_out[i * across + j] = chip_state[:, j * LANES : (j + 1) * LANES]
    tile_copies = [
        remote(tile_out.at[other], tile_in.at[chip], tile_send.at[i], tile_recv.at[i], mate(other))
        for i, other in enumerate(others)
    ]
    for copy in tile_copies:
        copy.start()
    tile_in[chip] = tile_out[chip]
    for copy in w_copies + w_loads:
        copy.start()

    lax.fori_loop(0, blocks, local, 0)

    for copy in sum_copies:
        copy.wait_recv()
    sums[...] = jnp.zeros_like(sums)
    for i in range(chips):
        sums[i : i + 1, :] = sum_in[i]
    spans[...] = jnp.exp(sums[...].T)
    mine_rows = pl.ds(pl.multiple_of(lax.div(chip, across) * ROWS, ROWS), ROWS)
    factors = spans[mine_rows, :]
    factor = [jnp.broadcast_to(factors[:, i : i + 1], (ROWS, LANES)) for i in range(chips)]
    for copy in tile_copies:
        copy.wait_recv()
    entering = jnp.zeros((ROWS, LANES), F32)
    for i in range(chips):
        enter_out[i] = entering.astype(BF16)
        entering = factor[i] * entering + tile_in[i].astype(F32)
    enter_copies = [
        remote(enter_out.at[other], enter_in.at[chip], enter_send.at[i], enter_recv.at[i], mate(other))
        for i, other in enumerate(others)
    ]
    for copy in enter_copies:
        copy.start()
    enter_in[chip] = enter_out[chip]

    for copy, hand in zip(w_copies, hand_copies):
        copy.wait_recv()
        hand.start()

    for copy in enter_copies:
        copy.wait_recv()
    for i in range(half // ROWS):
        rows = slice(i * ROWS, (i + 1) * ROWS)
        s0, _ = halves(rows)
        entry = jnp.concatenate(
            [enter_in[i * across + j] for j in range(across)], axis=1
        ).astype(F32)
        between = decays(0, rows) * entry + s0
        pass_out[rows, :] = jnp.where(first, between, entry).astype(BF16)
        carry[core, rows, :] = jnp.where(first, entry, between).astype(BF16)
    pass_copy = remote(pass_out, carry.at[core], pass_send.at[0], pass_recv.at[0], sibling)
    pass_copy.start()
    pass_copy.wait_recv()
    carried = carry[...].reshape(DK, DV)

    split = pieces // 2
    order = [i + j * split for i in range(split) for j in range(2)]
    parts = [slice(i * TOKENS, (i + 1) * TOKENS) for i in range(pieces)]
    g_copies = [
        remote(
            gated.at[0, parts[i], :], gated.at[1, parts[i], :], g_send.at[i], g_recv.at[i],
            near_a if i < split else near_b,
        )
        for i in range(pieces)
    ]
    y_copies = [
        remote(
            y_out.at[parts[i], :], y_in.at[parts[i], :], y_send.at[i], y_recv.at[i],
            near_b if i < split else near_a,
        )
        for i in range(pieces)
    ]
    for i in order:
        part = parts[i]
        a = att[part, :] + dot(qg[part, :], carried)
        spread = jnp.mean(a * a, axis=-1, keepdims=True)
        gated[0, part, :] = (a * lax.rsqrt(spread + 1e-05) * act[part, :]).astype(BF16)
        g_copies[i].start()
    for copy in w_loads:
        copy.wait()
    for copy in hand_copies:
        copy.wait_recv()
    for i in order:
        part = parts[i]
        g_copies[i].wait_recv()
        own_w, far_w = (w.at[2], w_a) if i < split else (w.at[1], w_b)
        y_out[part, :] = (
            dot(gated[0, part, :], own_w[...]) + dot(gated[1, part, :], far_w[1])
        ).astype(BF16)
        y_copies[i].start()
    for i in order:
        part = parts[i]
        far_w = w_a if i < split else w_b
        mine[part, :] = dot(gated[0, part, :], w[0]) + dot(gated[1, part, :], far_w[0])
    for i in order:
        part = parts[i]
        y_copies[i].wait_recv()
        out[part, :] = (mine[part, :] + y_in[part, :].astype(F32)).astype(BF16)

    for copy in (
        [log_copy, half_copy, pass_copy] + w_copies + hand_copies
        + sum_copies + tile_copies + enter_copies + g_copies + y_copies
    ):
        copy.wait_send()


def shards(n_seq, n_head, queries, key_vectors, values, log_gate, out_gate, norm_gain, out_weight):
    length = queries.shape[0]
    width = out_weight.shape[1] // n_head
    blocks = length // SPAN
    pieces = length // TOKENS
    chips = n_seq // 2
    half = DK // 2
    VM = pltpu.VMEM
    dma = pltpu.SemaphoreType.DMA
    tiles = VM((chips, ROWS, LANES), BF16)
    scratch = [
        VM((length, DK), BF16), VM((length, DK), BF16), VM((length, DV), BF16),
        VM((length, DK), BF16), VM((length, DV), BF16), VM((1, DV), F32),
        VM((3, DV, width), BF16), VM((2, DV, width), BF16), VM((2, DV, width), BF16),
        VM((blocks, SPAN, DK), F32), VM((blocks, DK), F32), VM((length, DK), BF16),
        VM((length, DK), BF16), VM((length, DV), F32), VM((length, DV), F32), VM((DK, DV), F32),
        VM((8, DK), F32), VM((8, DK), F32), VM((half, DV), BF16), VM((half, DV), BF16),
        VM((half, DV), F32), VM((2, half, 128), F32),
        VM((1, half), F32), VM((chips, 1, half), F32), VM((128, half), F32), VM((half, 128), F32),
        tiles, tiles, tiles, tiles, VM((half, DV), BF16), VM((2, half, DV), BF16),
        VM((2, length, DV), BF16), VM((length, width), F32),
        VM((length, width), BF16), VM((length, width), BF16),
        dma((6,)), dma((3,)), dma((2,)), dma((2,)), dma((2,)), dma((2,)),
        dma((1,)), dma((1,)), dma((1,)), dma((1,)), dma((1,)), dma((1,)),
        dma((chips - 1,)), dma((chips - 1,)), dma((chips - 1,)), dma((chips - 1,)),
        dma((chips - 1,)), dma((chips - 1,)),
        dma((pieces,)), dma((pieces,)), dma((pieces,)), dma((pieces,)),
    ]
    return pl.pallas_call(
        functools.partial(kernel, n_seq, n_head),
        out_shape=pltpu.VMEM((length, width), BF16),
        in_specs=[pl.BlockSpec(memory_space=pl.ANY)] * 7,
        out_specs=pl.BlockSpec(memory_space=pltpu.VMEM),
        scratch_shapes=scratch,
        compiler_params=pltpu.CompilerParams(
            collective_id=0, has_side_effects=True, vmem_limit_bytes=56 * 2**20
        ),
        name="gated_layer",
    )(queries, key_vectors, values, log_gate, out_gate, norm_gain.reshape(1, DV), out_weight)


def solution(mesh):
    in_specs = (
        P("seq", "head"),
        P("seq", "head"),
        P("seq", "head"),
        P("seq", "head"),
        P("seq", "head"),
        P("head"),
        P("head", None),
    )
    out_specs = P("seq", "head")
    body = functools.partial(shards, mesh.shape["seq"], mesh.shape["head"])
    return jax.shard_map(body, mesh=mesh, in_specs=in_specs, out_specs=out_specs, check_vma=False)
```

```python
import functools

import jax
import jax.numpy as jnp
from jax import lax
from jax.experimental import pallas as pl
from jax.experimental.pallas import tpu as pltpu
from jax.sharding import PartitionSpec as P

DK = 256
DV = 512
SPAN = 64
TOKENS = 64
Z = 8
F32 = jnp.float32
BF16 = jnp.bfloat16
MESH = pl.DeviceIdType.MESH


def dot(a, b, dims=((1,), (0,))):
    return lax.dot_general(a, b, (dims, ((), ())), preferred_element_type=F32)


def kernel(
    n_seq, n_head,
    q_hbm, k_hbm, v_hbm, g_hbm, o_hbm, gain_hbm, w_hbm,
    out,
    q, k, v, g, o, gain, w, w_a, w_b,
    run, ends, kd, qg, att, act, state,
    log_out, log_in, own_state, core_out, core_in, decay,
    sum_out, sum_in, row_out, row_in, sums, spans, row_spans,
    tile_out, tile_in, total_out, total_in, ahead, enter_out, enter_in, carry,
    gated, mine, y_out, y_in,
    load_sem, w_sem, w_send, w_recv, hand_send, hand_recv,
    log_send, log_recv, core_send, core_recv,
    sum_send, sum_recv, row_send, row_recv, tile_send, tile_recv,
    total_send, total_recv, enter_send, enter_recv, pass_send, pass_recv,
    g_send, g_recv, y_send, y_recv,
):
    length = q.shape[0]
    blocks = length // SPAN
    pieces = length // TOKENS
    width = w_hbm.shape[1] // n_head
    rows_x = n_seq // 2 // Z
    part_rows = DK // Z
    copies = DV // 128
    seq = lax.axis_index("seq")
    head = lax.axis_index("head")
    core = lax.rem(seq, 2)
    chip = lax.div(seq, 2)
    feeds = core == 0
    scans = core == 1
    at_x = lax.div(chip, Z)
    at_z = lax.rem(chip, Z)
    head_a = head + 1 - 2 * lax.rem(head, 2)
    head_b = n_head - 1 - head
    head_c = n_head - 1 - head_a
    sibling = {"seq": seq + 1 - 2 * core, "head": head}
    near_a = {"seq": seq, "head": head_a}
    near_b = {"seq": seq, "head": head_b}
    row_z = [lax.rem(at_z + dz, Z) for dz in sorted(range(1, Z), key=lambda d: abs(d - Z // 2))]
    from_z = [lax.rem(at_z + Z - dz, Z) for dz in sorted(range(1, Z), key=lambda d: abs(d - Z // 2))]

    def mate(x, z):
        return {"seq": (x * Z + z) * 2 + core, "head": head}

    in_row = [mate(at_x, z) for z in row_z]
    later = [mate(lax.rem(at_x + dx, rows_x), at_z) for dx in range(1, rows_x)]

    def columns(which):
        return pl.ds(pl.multiple_of(which * width, 128), width)

    def remote(src, dst, send, recv, device):
        return pltpu.make_async_remote_copy(
            src_ref=src, dst_ref=dst, send_sem=send, recv_sem=recv,
            device_id=device, device_id_type=MESH,
        )

    barrier = pltpu.get_barrier_semaphore()

    def greet(friends):
        for friend in friends:
            pl.semaphore_signal(barrier, inc=1, device_id=friend, device_id_type=MESH)

    near = [sibling, near_a, near_b]
    greet(near)
    pl.when(scans)(lambda: greet(in_row + later))
    loads = [
        pltpu.make_async_copy(src, dst, load_sem.at[i])
        for i, (src, dst) in enumerate(
            ((g_hbm, g), (k_hbm, k), (v_hbm, v), (q_hbm, q), (o_hbm, o), (gain_hbm, gain))
        )
    ]
    for load in loads:
        load.start()
    w_loads = [
        pltpu.make_async_copy(w_hbm.at[:, columns(which)], w.at[j], w_sem.at[j])
        for j, which in enumerate((head, head_a, head_b))
    ]
    w_copies = [
        remote(w_hbm.at[:, columns(which)], dst.at[j], w_send.at[i], w_recv.at[i], device)
        for i, (which, dst, j, device) in enumerate((
            (head_c, w_a, 1, near_a), (head_c, w_b, 1, near_b),
            (head_a, w_a, 0, near_a), (head_b, w_b, 0, near_b),
        ))
    ]
    hand_copies = [
        remote(dst.at[j], dst.at[j], hand_send.at[i], hand_recv.at[i], sibling)
        for i, (dst, j) in enumerate(((w_a, 1), (w_b, 1), (w_a, 0), (w_b, 0)))
    ]
    log_copy = remote(log_out, log_in, log_send.at[0], log_recv.at[0], sibling)
    core_copy = remote(core_out, core_in, core_send.at[0], core_recv.at[0], sibling)

    @pl.when(feeds)
    def _():
        pl.semaphore_wait(barrier, len(near))
        for copy in w_copies:
            copy.start()

    tri = (
        lax.broadcasted_iota(jnp.int32, (SPAN, SPAN), 0)
        >= lax.broadcasted_iota(jnp.int32, (SPAN, SPAN), 1)
    )
    ones = jnp.where(tri, 1.0, 0.0).astype(BF16)
    loads[0].wait()
    total = jnp.zeros((1, DK), F32)
    endings = []
    for b in range(blocks):
        r = dot(ones, g[b * SPAN : (b + 1) * SPAN, :])
        run[b] = r
        endings.append(r[SPAN - 1 : SPAN, :])
        ends[b : b + 1, :] = total
        total = total + endings[b]
    log_out[...] = total
    pl.when(feeds)(log_copy.start)
    loads[1].wait()
    tail = jnp.zeros((1, DK), F32)
    for b in reversed(range(blocks)):
        part = slice(b * SPAN, (b + 1) * SPAN)
        kd[part, :] = (k[part, :].astype(F32) * jnp.exp((endings[b] - run[b]) + tail)).astype(BF16)
        tail = tail + endings[b]
    loads[2].wait()
    for cols in (slice(0, DK // 2), slice(DK // 2, DK)):
        grown = dot(kd[:, cols], v[...], ((0,), (0,)))
        own_state[cols, :] = grown
        core_out[cols, :] = grown.astype(BF16)
    pl.when(feeds)(core_copy.start)
    for load in w_loads:
        load.start()

    def lanes(row):
        return jnp.broadcast_to(row, (128, DK)).T

    def wide(columns):
        return jnp.concatenate([columns] * copies, axis=1)

    def part_of(z):
        return slice(z * part_rows, (z + 1) * part_rows)

    sum_copies = [
        remote(sum_out, sum_in.at[at_z], sum_send.at[i], sum_recv.at[i], device)
        for i, device in enumerate(in_row)
    ]
    tile_copies = [
        remote(tile_out.at[z], tile_in.at[at_z], tile_send.at[i], tile_recv.at[i], device)
        for i, (z, device) in enumerate(zip(row_z, in_row))
    ]
    row_copies = [
        remote(row_out, row_in.at[at_x], row_send.at[i], row_recv.at[i], device)
        for i, device in enumerate(later)
    ]
    total_copies = [
        remote(total_out, total_in.at[at_x], total_send.at[i], total_recv.at[i], device)
        for i, device in enumerate(later)
    ]
    enter_copies = [
        remote(enter_out.at[z], enter_in.at[at_z], enter_send.at[i], enter_recv.at[i], device)
        for i, (z, device) in enumerate(zip(row_z, in_row))
    ]
    pass_copies = [
        remote(enter_in.at[z], carry.at[z], pass_send.at[i], pass_recv.at[i], sibling)
        for i, z in enumerate([at_z] + from_z)
    ]

    @pl.when(scans)
    def _():
        log_copy.wait_recv()
        sum_out[...] = log_out[...] + log_in[...]
        decay[0] = lanes(jnp.exp(log_in[...]))
        decay[1] = lanes(jnp.exp(log_out[...]))
        core_copy.wait_recv()
        for z in range(Z):
            part = part_of(z)
            tile_out[z] = (
                wide(decay[1, part, :]) * core_in[part, :].astype(F32) + own_state[part, :]
            ).astype(BF16)
        sum_in[at_z] = sum_out[...]
        tile_in[at_z] = tile_out[at_z]
        pl.semaphore_wait(barrier, len(near) + len(in_row) + len(later))
        for copy in sum_copies + tile_copies:
            copy.start()

    for load in loads[3:]:
        load.wait()
    state[...] = jnp.zeros_like(state)

    def local(b, _):
        part = pl.ds(pl.multiple_of(b * SPAN, SPAN), SPAN)
        r = run[b]
        middle = r[SPAN // 2 : SPAN // 2 + 1, :]
        ending = r[SPAN - 1 : SPAN, :]
        before = ends[pl.ds(b, 1), :]
        qf = q[part, :].astype(F32)
        kf = k[part, :].astype(F32)
        qi = qf * jnp.exp(r)
        qg[part, :] = (qi * jnp.exp(before)).astype(BF16)
        q_intra = (qf * jnp.exp(r - middle)).astype(BF16)
        k_intra = (kf * jnp.exp(middle - r)).astype(BF16)
        k_state = (kf * jnp.exp(ending - r)).astype(BF16)
        vb = v[part, :]
        scores = dot(q_intra, k_intra, ((1,), (1,)))
        weights = jnp.where(tri, scores, 0.0).astype(BF16)
        held = state[...]
        att[part, :] = dot(weights, vb) + dot(qi.astype(BF16), held.astype(BF16))
        state[...] = held * wide(lanes(jnp.exp(ending))) + dot(k_state, vb, ((0,), (0,)))
        of = o[part, :].astype(F32)
        act[part, :] = of / (1.0 + jnp.exp(-of)) * gain[...]
        return 0

    lax.fori_loop(0, blocks, local, 0)

    @pl.when(scans)
    def _():
        sums[...] = jnp.zeros_like(sums)
        for copy in sum_copies:
            copy.wait_recv()
        along = jnp.zeros((1, DK), F32)
        for z in range(Z):
            sums[z : z + 1, :] = sum_in[z]
            along = along + sum_in[z]
        row_out[...] = along
        for i, copy in enumerate(row_copies):
            pl.when(at_x + i + 1 < rows_x)(copy.start)
        spans[...] = jnp.exp(sums[...].T)
        own_rows = pl.ds(pl.multiple_of(at_z * part_rows, part_rows), part_rows)

        def factor(table, i):
            return wide(jnp.broadcast_to(table[own_rows, :][:, i : i + 1], (part_rows, 128)))

        for copy in tile_copies:
            copy.wait_recv()
        grown = tile_in[0].astype(F32)
        for z in range(1, Z):
            grown = factor(spans, z) * grown + tile_in[z].astype(F32)
        total_out[...] = grown.astype(BF16)
        for i, copy in enumerate(total_copies):
            pl.when(at_x + i + 1 < rows_x)(copy.start)
        ahead[...] = jnp.zeros_like(ahead)
        for x in range(rows_x - 1):

            @pl.when(at_x > x)
            def _():
                for i in range(rows_x - 1):
                    pl.when(at_x == x + i + 1)(row_copies[i].wait_recv)
                sums[Z + x : Z + x + 1, :] = row_in[x]

        @pl.when(at_x > 0)
        def _():
            row_spans[...] = jnp.exp(sums[...].T)

        for x in range(rows_x - 1):

            @pl.when(at_x > x)
            def _():
                for i in range(rows_x - 1):
                    pl.when(at_x == x + i + 1)(total_copies[i].wait_recv)
                ahead[...] = factor(row_spans, Z + x) * ahead[...] + total_in[x].astype(F32)

        entry = ahead[...]
        for z in range(Z):
            enter_out[z] = entry.astype(BF16)
            if z < Z - 1:
                entry = factor(spans, z) * entry + tile_in[z].astype(F32)
        for copy in enter_copies:
            copy.start()
        enter_in[at_z] = enter_out[at_z]
        pass_copies[0].start()
        for copy, onward in zip(enter_copies, pass_copies[1:]):
            copy.wait_recv()
            onward.start()
        for z in range(Z):
            part = part_of(z)
            carry[z] = (
                wide(decay[0, part, :]) * enter_in[z].astype(F32) + core_in[part, :].astype(F32)
            ).astype(BF16)

    @pl.when(feeds)
    def _():
        for copy, hand in zip(w_copies, hand_copies):
            copy.wait_recv()
            hand.start()
        for copy in pass_copies:
            copy.wait_recv()

    carried = carry[...].reshape(DK, DV)

    split = pieces // 2
    order = [i + j * split for i in range(split) for j in range(2)]
    parts = [slice(i * TOKENS, (i + 1) * TOKENS) for i in range(pieces)]
    g_copies = [
        remote(
            gated.at[0, parts[i], :], gated.at[1, parts[i], :], g_send.at[i], g_recv.at[i],
            near_a if i < split else near_b,
        )
        for i in range(pieces)
    ]
    y_copies = [
        remote(
            y_out.at[parts[i], :], y_in.at[parts[i], :], y_send.at[i], y_recv.at[i],
            near_b if i < split else near_a,
        )
        for i in range(pieces)
    ]
    for i in order:
        part = parts[i]
        a = att[part, :] + dot(qg[part, :], carried)
        spread = jnp.mean(a * a, axis=-1, keepdims=True)
        gated[0, part, :] = (a * lax.rsqrt(spread + 1e-05) * act[part, :]).astype(BF16)
        g_copies[i].start()
    for copy in w_loads:
        copy.wait()

    @pl.when(scans)
    def _():
        for copy in hand_copies:
            copy.wait_recv()

    for i in order:
        part = parts[i]
        g_copies[i].wait_recv()
        own_w, far_w = (w.at[2], w_a) if i < split else (w.at[1], w_b)
        y_out[part, :] = (
            dot(gated[0, part, :], own_w[...]) + dot(gated[1, part, :], far_w[1])
        ).astype(BF16)
        y_copies[i].start()
    for i in order:
        part = parts[i]
        far_w = w_a if i < split else w_b
        mine[part, :] = dot(gated[0, part, :], w[0]) + dot(gated[1, part, :], far_w[0])
    for i in order:
        part = parts[i]
        y_copies[i].wait_recv()
        out[part, :] = (mine[part, :] + y_in[part, :].astype(F32)).astype(BF16)

    for copy in g_copies + y_copies:
        copy.wait_send()

    @pl.when(feeds)
    def _():
        for copy in [log_copy, core_copy] + w_copies + hand_copies:
            copy.wait_send()

    @pl.when(scans)
    def _():
        for copy in sum_copies + tile_copies + enter_copies + pass_copies:
            copy.wait_send()
        for i in range(rows_x - 1):

            @pl.when(at_x + i + 1 < rows_x)
            def _():
                row_copies[i].wait_send()
                total_copies[i].wait_send()


def shards(n_seq, n_head, queries, key_vectors, values, log_gate, out_gate, norm_gain, out_weight):
    length = queries.shape[0]
    width = out_weight.shape[1] // n_head
    blocks = length // SPAN
    pieces = length // TOKENS
    rows_x = n_seq // 2 // Z
    VM = pltpu.VMEM
    dma = pltpu.SemaphoreType.DMA
    tiles = VM((Z, DK // Z, DV), BF16)
    row = VM((1, DK), F32)
    scratch = [
        VM((length, DK), BF16), VM((length, DK), BF16), VM((length, DV), BF16),
        VM((length, DK), BF16), VM((length, DV), BF16), VM((1, DV), F32),
        VM((3, DV, width), BF16), VM((2, DV, width), BF16), VM((2, DV, width), BF16),
        VM((blocks, SPAN, DK), F32), VM((blocks, DK), F32), VM((length, DK), BF16),
        VM((length, DK), BF16), VM((length, DV), F32), VM((length, DV), F32), VM((DK, DV), F32),
        row, row, VM((DK, DV), F32), VM((DK, DV), BF16), VM((DK, DV), BF16), VM((2, DK, 128), F32),
        row, VM((Z, 1, DK), F32), row, VM((rows_x, 1, DK), F32),
        VM((128, DK), F32), VM((DK, 128), F32), VM((DK, 128), F32),
        tiles, tiles, VM((DK // Z, DV), BF16), VM((rows_x, DK // Z, DV), BF16),
        VM((DK // Z, DV), F32), tiles, tiles, tiles,
        VM((2, length, DV), BF16), VM((length, width), F32),
        VM((length, width), BF16), VM((length, width), BF16),
        dma((6,)), dma((3,)), dma((4,)), dma((4,)), dma((4,)), dma((4,)),
        dma((1,)), dma((1,)), dma((1,)), dma((1,)),
        dma((Z - 1,)), dma((Z - 1,)), dma((rows_x - 1,)), dma((rows_x - 1,)),
        dma((Z - 1,)), dma((Z - 1,)), dma((rows_x - 1,)), dma((rows_x - 1,)),
        dma((Z - 1,)), dma((Z - 1,)), dma((Z,)), dma((Z,)),
        dma((pieces,)), dma((pieces,)), dma((pieces,)), dma((pieces,)),
    ]
    return pl.pallas_call(
        functools.partial(kernel, n_seq, n_head),
        out_shape=pltpu.VMEM((length, width), BF16),
        in_specs=[pl.BlockSpec(memory_space=pl.ANY)] * 7,
        out_specs=pl.BlockSpec(memory_space=pltpu.VMEM),
        scratch_shapes=scratch,
        compiler_params=pltpu.CompilerParams(
            collective_id=0, has_side_effects=True, vmem_limit_bytes=56 * 2**20
        ),
        name="gated_layer",
    )(queries, key_vectors, values, log_gate, out_gate, norm_gain.reshape(1, DV), out_weight)


def solution(mesh):
    in_specs = (
        P("seq", "head"),
        P("seq", "head"),
        P("seq", "head"),
        P("seq", "head"),
        P("seq", "head"),
        P("head"),
        P("head", None),
    )
    out_specs = P("seq", "head")
    body = functools.partial(shards, mesh.shape["seq"], mesh.shape["head"])
    return jax.shard_map(body, mesh=mesh, in_specs=in_specs, out_specs=out_specs, check_vma=False)
```

```python
import functools

import jax
import jax.numpy as jnp
from jax import lax
from jax.experimental import pallas as pl
from jax.experimental.pallas import tpu as pltpu
from jax.sharding import PartitionSpec as P

DK = 256
DV = 512
SPAN = 64
TOKENS = 64
Z = 8
F32 = jnp.float32
BF16 = jnp.bfloat16
MESH = pl.DeviceIdType.MESH


def dot(a, b, dims=((1,), (0,))):
    return lax.dot_general(a, b, (dims, ((), ())), preferred_element_type=F32)


def kernel(
    n_seq, n_head,
    q_hbm, k_hbm, v_hbm, g_hbm, o_hbm, gain_hbm, w_hbm,
    out,
    q, k, v, g, o, gain, w, w_near,
    run, ends, kd, qg, att, act, state,
    log_out, log_in, own_state, core_out, core_in, decay,
    sum_out, sum_in, row_out, row_in, sums, spans, row_spans,
    tile_out, tile_in, total_out, total_in, ahead, enter_out, enter_in, carry,
    gated, mine, y_out, y_in,
    load_sem, w_sem, w_send, w_recv, hand_send, hand_recv,
    log_send, log_recv, core_send, core_recv,
    sum_send, sum_recv, row_send, row_recv, tile_send, tile_recv,
    total_send, total_recv, enter_send, enter_recv, pass_send, pass_recv,
    g_send, g_recv, y_send, y_recv,
):
    loads = [
        pltpu.make_async_copy(src, dst, load_sem.at[i])
        for i, (src, dst) in enumerate(
            ((g_hbm, g), (k_hbm, k), (v_hbm, v), (q_hbm, q), (o_hbm, o), (gain_hbm, gain))
        )
    ]
    for load in loads[:3]:
        load.start()
    length = q.shape[0]
    blocks = length // SPAN
    pieces = length // TOKENS
    width = w_hbm.shape[1] // n_head
    rows_x = n_seq // 2 // Z
    part_rows = DK // Z
    copies = DV // 128
    seq = lax.axis_index("seq")
    head = lax.axis_index("head")
    core = lax.rem(seq, 2)
    chip = lax.div(seq, 2)
    feeds = core == 0
    scans = core == 1
    at_x = lax.div(chip, Z)
    at_z = lax.rem(chip, Z)
    head_a = head + 1 - 2 * lax.rem(head, 2)
    head_b = n_head - 1 - head
    head_c = n_head - 1 - head_a
    sibling = {"seq": seq + 1 - 2 * core, "head": head}
    near_a = {"seq": seq, "head": head_a}
    near_b = {"seq": seq, "head": head_b}

    def mate(x, z):
        return {"seq": (x * Z + z) * 2 + core, "head": head}

    in_row = [mate(at_x, lax.rem(at_z + dz, Z)) for dz in range(1, Z)]
    later = {dx: mate(lax.rem(at_x + dx, rows_x), at_z) for dx in (2, 1, 3)}

    def columns(which):
        return pl.ds(pl.multiple_of(which * width, 128), width)

    def remote(src, dst, send, recv, device):
        return pltpu.make_async_remote_copy(
            src_ref=src, dst_ref=dst, send_sem=send, recv_sem=recv,
            device_id=device, device_id_type=MESH,
        )

    def landed(ref, sem):
        pltpu.make_async_copy(ref, ref, sem).wait()

    barrier = pltpu.get_barrier_semaphore()

    def greet(friends):
        for friend in friends:
            pl.semaphore_signal(barrier, inc=1, device_id=friend, device_id_type=MESH)

    near = [sibling, near_a, near_b]
    greet(near)
    pl.when(scans)(lambda: greet(in_row + list(later.values())))
    w_loads = [
        pltpu.make_async_copy(w_hbm.at[:, columns(which)], w.at[j], w_sem.at[0])
        for j, which in enumerate((head, head_a, head_b))
    ]
    w_copies = [
        remote(w_hbm.at[:, columns(which)], w_near.at[j, i], w_send.at[0], w_recv.at[j], device)
        for which, j, i, device in (
            (head_c, 1, 0, near_a), (head_c, 1, 1, near_b),
            (head_a, 0, 0, near_a), (head_b, 0, 1, near_b),
        )
    ]
    hand_copies = [
        remote(w_near.at[j], w_near.at[j], hand_send.at[0], hand_recv.at[0], sibling) for j in (1, 0)
    ]
    log_copy = remote(log_out, log_in, log_send.at[0], log_recv.at[0], sibling)
    channels = [slice(0, DK // 2), slice(DK // 2, DK)]
    core_copies = [
        remote(core_out.at[cols, :], core_in.at[cols, :], core_send.at[0], core_recv.at[i], sibling)
        for i, cols in enumerate(channels)
    ]

    tri = (
        lax.broadcasted_iota(jnp.int32, (SPAN, SPAN), 0)
        >= lax.broadcasted_iota(jnp.int32, (SPAN, SPAN), 1)
    )
    ones = jnp.where(tri, 1.0, 0.0).astype(BF16)
    loads[0].wait()
    total = jnp.zeros((1, DK), F32)
    endings = []
    for b in range(blocks):
        r = dot(ones, g[b * SPAN : (b + 1) * SPAN, :])
        run[b] = r
        endings.append(r[SPAN - 1 : SPAN, :])
        ends[b : b + 1, :] = total
        total = total + endings[b]
    log_out[...] = total
    loads[1].wait()
    tail = jnp.zeros((1, DK), F32)
    for b in reversed(range(blocks)):
        part = slice(b * SPAN, (b + 1) * SPAN)
        kd[part, :] = (k[part, :].astype(F32) * jnp.exp((endings[b] - run[b]) + tail)).astype(BF16)
        tail = tail + endings[b]
    loads[2].wait()

    @pl.when(feeds)
    def _():
        pl.semaphore_wait(barrier, len(near))
        log_copy.start()

    for cols, core_copy in zip(channels, core_copies):
        grown = dot(kd[:, cols], v[...], ((0,), (0,)))
        own_state[cols, :] = grown
        core_out[cols, :] = grown.astype(BF16)
        pl.when(feeds)(core_copy.start)
    for load in loads[3:] + w_loads:
        load.start()

    @pl.when(feeds)
    def _():
        for copy in w_copies:
            copy.start()

    def lanes(row):
        return jnp.broadcast_to(row, (128, DK)).T

    def wide(columns):
        return jnp.concatenate([columns] * copies, axis=1)

    def part_of(z):
        return slice(z * part_rows, (z + 1) * part_rows)

    sum_copies = [
        remote(sum_out, sum_in.at[at_z], sum_send.at[0], sum_recv.at[0], device)
        for device in in_row
    ]
    tile_copies = [
        remote(tile_out.at[z], tile_in.at[at_z], tile_send.at[0], tile_recv.at[0], mate(at_x, z))
        for z in range(Z)
    ]
    row_copies = {
        dx: remote(row_out, row_in.at[at_x], row_send.at[0], row_recv.at[0], device)
        for dx, device in later.items()
    }
    total_copies = {
        dx: remote(total_out, total_in.at[at_x], total_send.at[0], total_recv.at[0], device)
        for dx, device in later.items()
    }
    enter_copies = [
        remote(enter_out.at[z], enter_in.at[at_z], enter_send.at[0], enter_recv.at[0], mate(at_x, z))
        for z in range(Z)
    ]
    pass_copy = remote(enter_in, carry, pass_send.at[0], pass_recv.at[0], sibling)

    @pl.when(scans)
    def _():
        log_copy.wait_recv()
        sum_out[...] = log_out[...] + log_in[...]
        decay[0] = lanes(jnp.exp(log_in[...]))
        decay[1] = lanes(jnp.exp(log_out[...]))
        sum_in[at_z] = sum_out[...]
        pl.semaphore_wait(barrier, len(near) + len(in_row) + len(later))
        for copy in sum_copies:
            copy.start()
        for i, core_copy in enumerate(core_copies):
            core_copy.wait_recv()
            for z in range(i * Z // 2, (i + 1) * Z // 2):
                part = part_of(z)
                tile_out[z] = (
                    wide(decay[1, part, :]) * core_in[part, :].astype(F32) + own_state[part, :]
                ).astype(BF16)
            for z in range(i * Z // 2, (i + 1) * Z // 2):
                pl.when(at_z != z)(tile_copies[z].start)
        tile_in[at_z] = tile_out[at_z]

    for load in loads[3:]:
        load.wait()
    state[...] = jnp.zeros_like(state)

    def local(b, _):
        part = pl.ds(pl.multiple_of(b * SPAN, SPAN), SPAN)
        r = run[b]
        middle = r[SPAN // 2 : SPAN // 2 + 1, :]
        ending = r[SPAN - 1 : SPAN, :]
        before = ends[pl.ds(b, 1), :]
        qf = q[part, :].astype(F32)
        kf = k[part, :].astype(F32)
        qi = qf * jnp.exp(r)
        qg[part, :] = (qi * jnp.exp(before)).astype(BF16)
        q_intra = (qf * jnp.exp(r - middle)).astype(BF16)
        k_intra = (kf * jnp.exp(middle - r)).astype(BF16)
        k_state = (kf * jnp.exp(ending - r)).astype(BF16)
        vb = v[part, :]
        scores = dot(q_intra, k_intra, ((1,), (1,)))
        weights = jnp.where(tri, scores, 0.0).astype(BF16)
        held = state[...]
        att[part, :] = dot(weights, vb) + dot(qi.astype(BF16), held.astype(BF16))
        state[...] = held * wide(lanes(jnp.exp(ending))) + dot(k_state, vb, ((0,), (0,)))
        of = o[part, :].astype(F32)
        act[part, :] = of / (1.0 + jnp.exp(-of)) * gain[...]
        return 0

    lax.fori_loop(0, blocks, local, 0)

    @pl.when(scans)
    def _():
        sums[...] = jnp.zeros_like(sums)
        landed(sum_in.at[0 : Z - 1], sum_recv.at[0])
        along = jnp.zeros((1, DK), F32)
        for z in range(Z):
            sums[z : z + 1, :] = sum_in[z]
            along = along + sum_in[z]
        row_out[...] = along
        for dx, copy in row_copies.items():
            pl.when(at_x + dx < rows_x)(copy.start)
        spans[...] = jnp.exp(sums[...].T)
        own_rows = pl.ds(pl.multiple_of(at_z * part_rows, part_rows), part_rows)

        def factor(table, i):
            return wide(jnp.broadcast_to(table[own_rows, :][:, i : i + 1], (part_rows, 128)))

        landed(tile_in.at[0 : Z - 1], tile_recv.at[0])
        grown = tile_in[0].astype(F32)
        for z in range(1, Z):
            grown = factor(spans, z) * grown + tile_in[z].astype(F32)
        total_out[...] = grown.astype(BF16)
        for dx, copy in total_copies.items():
            pl.when(at_x + dx < rows_x)(copy.start)
        ahead[...] = jnp.zeros_like(ahead)
        for x in range(1, rows_x):

            @pl.when(at_x == x)
            def _():
                landed(row_in.at[0:x], row_recv.at[0])
                for i in range(x):
                    sums[Z + i : Z + i + 1, :] = row_in[i]
                row_spans[...] = jnp.exp(sums[...].T)
                landed(total_in.at[0:x], total_recv.at[0])
                gone = total_in[0].astype(F32)
                for i in range(1, x):
                    gone = factor(row_spans, Z + i) * gone + total_in[i].astype(F32)
                ahead[...] = gone

        entry = ahead[...]
        for z in range(Z):
            enter_out[z] = entry.astype(BF16)
            if z < Z - 1:
                entry = factor(spans, z) * entry + tile_in[z].astype(F32)
        for z, copy in enumerate(enter_copies):
            pl.when(at_z != z)(copy.start)
        enter_in[at_z] = enter_out[at_z]
        landed(enter_in.at[0 : Z - 1], enter_recv.at[0])
        pass_copy.start()
        for z in range(Z):
            part = part_of(z)
            carry[z] = (
                wide(decay[0, part, :]) * enter_in[z].astype(F32) + core_in[part, :].astype(F32)
            ).astype(BF16)

    @pl.when(feeds)
    def _():
        for j, hand in zip((1, 0), hand_copies):
            landed(w_near.at[j], w_recv.at[j])
            hand.start()
        pass_copy.wait_recv()

    carried = carry[...].reshape(DK, DV)

    split = pieces // 2
    order = [i + j * split for i in range(split) for j in range(2)]
    parts = [slice(i * TOKENS, (i + 1) * TOKENS) for i in range(pieces)]
    g_copies = [
        remote(
            gated.at[0, parts[i], :], gated.at[1, parts[i], :], g_send.at[0], g_recv.at[i],
            near_a if i < split else near_b,
        )
        for i in range(pieces)
    ]
    y_copies = [
        remote(
            y_out.at[parts[i], :], y_in.at[parts[i], :], y_send.at[0], y_recv.at[i // 2],
            near_b if i < split else near_a,
        )
        for i in range(pieces)
    ]
    for i in order:
        part = parts[i]
        a = att[part, :] + dot(qg[part, :], carried)
        spread = jnp.mean(a * a, axis=-1, keepdims=True)
        gated[0, part, :] = (a * lax.rsqrt(spread + 1e-05) * act[part, :]).astype(BF16)
        g_copies[i].start()
    landed(w, w_sem.at[0])
    pl.when(scans)(lambda: landed(w_near, hand_recv.at[0]))

    for i in order:
        part = parts[i]
        g_copies[i].wait_recv()
        j = i // split
        y_out[part, :] = (
            dot(gated[0, part, :], w[2 - j]) + dot(gated[1, part, :], w_near[1, j])
        ).astype(BF16)
        y_copies[i].start()
    for i in order:
        part = parts[i]
        mine[part, :] = dot(gated[0, part, :], w[0]) + dot(gated[1, part, :], w_near[0, i // split])
    for i in (0, 2, 1, 3):
        part = slice(2 * i * TOKENS, 2 * (i + 1) * TOKENS)
        landed(y_in.at[part, :], y_recv.at[i])
        out[part, :] = (mine[part, :] + y_in[part, :].astype(F32)).astype(BF16)

    landed(gated.at[0], g_send.at[0])
    landed(y_out, y_send.at[0])

    @pl.when(feeds)
    def _():
        log_copy.wait_send()
        landed(core_out, core_send.at[0])
        landed(w_near, w_send.at[0])
        landed(w_near, hand_send.at[0])

    @pl.when(scans)
    def _():
        landed(sum_in.at[0 : Z - 1], sum_send.at[0])
        landed(tile_out.at[0 : Z - 1], tile_send.at[0])
        landed(enter_out.at[0 : Z - 1], enter_send.at[0])
        pass_copy.wait_send()
        for x in range(rows_x - 1):

            @pl.when(at_x == x)
            def _():
                landed(row_in.at[0 : rows_x - 1 - x], row_send.at[0])
                landed(total_in.at[0 : rows_x - 1 - x], total_send.at[0])


def shards(n_seq, n_head, queries, key_vectors, values, log_gate, out_gate, norm_gain, out_weight):
    length = queries.shape[0]
    width = out_weight.shape[1] // n_head
    blocks = length // SPAN
    pieces = length // TOKENS
    rows_x = n_seq // 2 // Z
    VM = pltpu.VMEM
    dma = pltpu.SemaphoreType.DMA
    tiles = VM((Z, DK // Z, DV), BF16)
    row = VM((1, DK), F32)
    scratch = [
        VM((length, DK), BF16), VM((length, DK), BF16), VM((length, DV), BF16),
        VM((length, DK), BF16), VM((length, DV), BF16), VM((1, DV), F32),
        VM((3, DV, width), BF16), VM((2, 2, DV, width), BF16),
        VM((blocks, SPAN, DK), F32), VM((blocks, DK), F32), VM((length, DK), BF16),
        VM((length, DK), BF16), VM((length, DV), F32), VM((length, DV), F32), VM((DK, DV), F32),
        row, row, VM((DK, DV), F32), VM((DK, DV), BF16), VM((DK, DV), BF16), VM((2, DK, 128), F32),
        row, VM((Z, 1, DK), F32), row, VM((rows_x, 1, DK), F32),
        VM((128, DK), F32), VM((DK, 128), F32), VM((DK, 128), F32),
        tiles, tiles, VM((DK // Z, DV), BF16), VM((rows_x, DK // Z, DV), BF16),
        VM((DK // Z, DV), F32), tiles, tiles, tiles,
        VM((2, length, DV), BF16), VM((length, width), F32),
        VM((length, width), BF16), VM((length, width), BF16),
        dma((6,)), dma((1,)), dma((1,)), dma((2,)), dma((1,)), dma((1,)),
        dma((1,)), dma((1,)), dma((1,)), dma((2,)),
        dma((1,)), dma((1,)), dma((1,)), dma((1,)), dma((1,)), dma((1,)),
        dma((1,)), dma((1,)), dma((1,)), dma((1,)), dma((1,)), dma((1,)),
        dma((1,)), dma((pieces,)), dma((1,)), dma((pieces // 2,)),
    ]
    return pl.pallas_call(
        functools.partial(kernel, n_seq, n_head),
        out_shape=pltpu.VMEM((length, width), BF16),
        in_specs=[pl.BlockSpec(memory_space=pl.ANY)] * 7,
        out_specs=pl.BlockSpec(memory_space=pltpu.VMEM),
        scratch_shapes=scratch,
        compiler_params=pltpu.CompilerParams(
            collective_id=0, has_side_effects=True, vmem_limit_bytes=56 * 2**20
        ),
        name="gated_layer",
    )(queries, key_vectors, values, log_gate, out_gate, norm_gain.reshape(1, DV), out_weight)


def solution(mesh):
    in_specs = (
        P("seq", "head"),
        P("seq", "head"),
        P("seq", "head"),
        P("seq", "head"),
        P("seq", "head"),
        P("head"),
        P("head", None),
    )
    out_specs = P("seq", "head")
    body = functools.partial(shards, mesh.shape["seq"], mesh.shape["head"])
    return jax.shard_map(body, mesh=mesh, in_specs=in_specs, out_specs=out_specs, check_vma=False)
```

```python
import functools

import jax
import jax.numpy as jnp
from jax import lax
from jax.experimental import pallas as pl
from jax.experimental.pallas import tpu as pltpu
from jax.sharding import PartitionSpec as P

DK = 256
DV = 512
SPAN = 64
TOKENS = 128
Z = 8
EARLY = 3
F32 = jnp.float32
BF16 = jnp.bfloat16
MESH = pl.DeviceIdType.MESH


def dot(a, b, dims=((1,), (0,))):
    return lax.dot_general(a, b, (dims, ((), ())), preferred_element_type=F32)


def kernel(
    n_seq, n_head,
    q_hbm, k_hbm, v_hbm, g_hbm, o_hbm, gain_hbm, w_hbm,
    out,
    q, k, v, g, o, gain, w, w_near,
    run, ends, kd, qg, att, act, state,
    log_out, log_in, own_state, core_out, core_in, decay,
    sum_out, sum_in, row_out, row_in, sums, spans, row_spans,
    tile_out, tile_in, total_out, total_in, ahead, enter_out, enter_in, carry,
    gated, mine, y_out, y_in,
    load_sem, w_sem, w_send, w_recv, hand_send, hand_recv,
    log_send, log_recv, core_send, core_recv,
    sum_send, sum_recv, row_send, row_recv, tile_send, tile_recv,
    total_send, total_recv, enter_send, enter_recv, pass_send, pass_recv,
    g_send, g_recv, y_send, y_recv,
):
    loads = [
        pltpu.make_async_copy(src, dst, load_sem.at[i])
        for i, (src, dst) in enumerate(
            ((g_hbm, g), (k_hbm, k), (v_hbm, v), (q_hbm, q), (o_hbm, o), (gain_hbm, gain))
        )
    ]
    for load in loads[:3]:
        load.start()
    length = q.shape[0]
    blocks = length // SPAN
    pieces = length // TOKENS
    width = w_hbm.shape[1] // n_head
    rows_x = n_seq // 2 // Z
    part_rows = DK // Z
    copies = DV // 128
    seq = lax.axis_index("seq")
    head = lax.axis_index("head")
    core = lax.rem(seq, 2)
    chip = lax.div(seq, 2)
    feeds = core == 0
    scans = core == 1
    at_x = lax.div(chip, Z)
    at_z = lax.rem(chip, Z)
    head_a = head + 1 - 2 * lax.rem(head, 2)
    head_b = n_head - 1 - head
    head_c = n_head - 1 - head_a
    sibling = {"seq": seq + 1 - 2 * core, "head": head}
    near_a = {"seq": seq, "head": head_a}
    near_b = {"seq": seq, "head": head_b}

    def mate(x, z):
        return {"seq": (x * Z + z) * 2 + core, "head": head}

    in_row = [mate(at_x, lax.rem(at_z + dz, Z)) for dz in range(1, Z)]
    later = {dx: mate(lax.rem(at_x + dx, rows_x), at_z) for dx in (2, 1, 3)}

    def columns(which):
        return pl.ds(pl.multiple_of(which * width, 128), width)

    def remote(src, dst, send, recv, device):
        return pltpu.make_async_remote_copy(
            src_ref=src, dst_ref=dst, send_sem=send, recv_sem=recv,
            device_id=device, device_id_type=MESH,
        )

    def landed(ref, sem):
        pltpu.make_async_copy(ref, ref, sem).wait()

    barrier = pltpu.get_barrier_semaphore()

    def greet(friends):
        for friend in friends:
            pl.semaphore_signal(barrier, inc=1, device_id=friend, device_id_type=MESH)

    near = [sibling, near_a, near_b]
    greet(near)
    pl.when(scans)(lambda: greet(in_row + list(later.values())))
    w_loads = [
        pltpu.make_async_copy(w_hbm.at[:, columns(which)], w.at[j], w_sem.at[0])
        for j, which in enumerate((head, head_a, head_b))
    ]
    w_copies = [
        remote(w_hbm.at[:, columns(which)], w_near.at[j, i], w_send.at[0], w_recv.at[j], device)
        for which, j, i, device in (
            (head_c, 1, 0, near_a), (head_c, 1, 1, near_b),
            (head_a, 0, 0, near_a), (head_b, 0, 1, near_b),
        )
    ]
    hand_copies = [
        remote(w_near.at[j], w_near.at[j], hand_send.at[0], hand_recv.at[0], sibling) for j in (1, 0)
    ]
    log_copy = remote(log_out, log_in, log_send.at[0], log_recv.at[0], sibling)
    channels = [slice(0, DK // 2), slice(DK // 2, DK)]
    core_copies = [
        remote(core_out.at[cols, :], core_in.at[cols, :], core_send.at[0], core_recv.at[i], sibling)
        for i, cols in enumerate(channels)
    ]

    tri = (
        lax.broadcasted_iota(jnp.int32, (SPAN, SPAN), 0)
        >= lax.broadcasted_iota(jnp.int32, (SPAN, SPAN), 1)
    )
    ones = jnp.where(tri, 1.0, 0.0).astype(BF16)
    loads[0].wait()
    total = jnp.zeros((1, DK), F32)
    endings = []
    for b in range(blocks):
        r = dot(ones, g[b * SPAN : (b + 1) * SPAN, :])
        run[b] = r
        endings.append(r[SPAN - 1 : SPAN, :])
        ends[b : b + 1, :] = total
        total = total + endings[b]
    log_out[...] = total
    loads[1].wait()
    tail = jnp.zeros((1, DK), F32)
    for b in reversed(range(blocks)):
        part = slice(b * SPAN, (b + 1) * SPAN)
        kd[part, :] = (k[part, :].astype(F32) * jnp.exp((endings[b] - run[b]) + tail)).astype(BF16)
        tail = tail + endings[b]
    loads[2].wait()

    @pl.when(feeds)
    def _():
        pl.semaphore_wait(barrier, len(near))
        log_copy.start()

    for cols, core_copy in zip(channels, core_copies):
        grown = dot(kd[:, cols], v[...], ((0,), (0,)))
        own_state[cols, :] = grown
        core_out[cols, :] = grown.astype(BF16)
        pl.when(feeds)(core_copy.start)
    for load in loads[3:] + w_loads:
        load.start()

    @pl.when(feeds)
    def _():
        for copy in w_copies:
            copy.start()

    def lanes(row):
        return jnp.broadcast_to(row, (128, DK)).T

    def wide(columns):
        return jnp.concatenate([columns] * copies, axis=1)

    def part_of(z):
        return slice(z * part_rows, (z + 1) * part_rows)

    sum_copies = [
        remote(sum_out, sum_in.at[at_z], sum_send.at[0], sum_recv.at[0], device)
        for device in in_row
    ]
    far_first = [lax.rem(at_z + dz, Z) for dz in (4, 3, 5, 2, 6, 1, 7)]
    tile_copies = [
        remote(tile_out.at[z], tile_in.at[at_z], tile_send.at[0], tile_recv.at[0], mate(at_x, z))
        for z in far_first
    ]
    row_copies = {
        dx: remote(row_out, row_in.at[at_x], row_send.at[0], row_recv.at[0], device)
        for dx, device in later.items()
    }
    total_copies = {
        dx: remote(total_out, total_in.at[at_x], total_send.at[0], total_recv.at[0], device)
        for dx, device in later.items()
    }
    enter_copies = [
        remote(enter_out.at[z], enter_in.at[at_z], enter_send.at[0], enter_recv.at[0], mate(at_x, z))
        for z in list(range(EARLY)) + far_first
    ]
    pass_copy = remote(enter_in, carry, pass_send.at[0], pass_recv.at[0], sibling)

    @pl.when(scans)
    def _():
        log_copy.wait_recv()
        sum_out[...] = log_out[...] + log_in[...]
        decay[0] = lanes(jnp.exp(log_in[...]))
        decay[1] = lanes(jnp.exp(log_out[...]))
        sum_in[at_z] = sum_out[...]
        pl.semaphore_wait(barrier, len(near) + len(in_row) + len(later))
        for copy in sum_copies:
            copy.start()
        for i, core_copy in enumerate(core_copies):
            core_copy.wait_recv()
            for z in range(i * Z // 2, (i + 1) * Z // 2):
                part = part_of(z)
                tile_out[z] = (
                    wide(decay[1, part, :]) * core_in[part, :].astype(F32) + own_state[part, :]
                ).astype(BF16)
        for copy in tile_copies:
            copy.start()
        tile_in[at_z] = tile_out[at_z]

    for load in loads[3:]:
        load.wait()
    state[...] = jnp.zeros_like(state)

    def local(b, _):
        part = pl.ds(pl.multiple_of(b * SPAN, SPAN), SPAN)
        r = run[b]
        middle = r[SPAN // 2 : SPAN // 2 + 1, :]
        ending = r[SPAN - 1 : SPAN, :]
        before = ends[pl.ds(b, 1), :]
        qf = q[part, :].astype(F32)
        kf = k[part, :].astype(F32)
        qi = qf * jnp.exp(r)
        qg[part, :] = (qi * jnp.exp(before)).astype(BF16)
        q_intra = (qf * jnp.exp(r - middle)).astype(BF16)
        k_intra = (kf * jnp.exp(middle - r)).astype(BF16)
        k_state = (kf * jnp.exp(ending - r)).astype(BF16)
        vb = v[part, :]
        scores = dot(q_intra, k_intra, ((1,), (1,)))
        weights = jnp.where(tri, scores, 0.0).astype(BF16)
        held = state[...]
        att[part, :] = dot(weights, vb) + dot(qi.astype(BF16), held.astype(BF16))
        state[...] = held * wide(lanes(jnp.exp(ending))) + dot(k_state, vb, ((0,), (0,)))
        of = o[part, :].astype(F32)
        act[part, :] = of / (1.0 + jnp.exp(-of)) * gain[...]
        return 0

    lax.fori_loop(0, blocks, local, 0)

    @pl.when(scans)
    def _():
        sums[...] = jnp.zeros_like(sums)
        landed(sum_in.at[0 : Z - 1], sum_recv.at[0])
        along = jnp.zeros((1, DK), F32)
        for z in range(Z):
            sums[z : z + 1, :] = sum_in[z]
            along = along + sum_in[z]
        row_out[...] = along
        for dx, copy in row_copies.items():
            pl.when(at_x + dx < rows_x)(copy.start)
        spans[...] = jnp.exp(sums[...].T)
        own_rows = pl.ds(pl.multiple_of(at_z * part_rows, part_rows), part_rows)

        def factor(table, i):
            return wide(jnp.broadcast_to(table[own_rows, :][:, i : i + 1], (part_rows, 128)))

        landed(tile_in.at[0 : Z - 1], tile_recv.at[0])
        grown = tile_in[0].astype(F32)
        for z in range(1, Z):
            grown = factor(spans, z) * grown + tile_in[z].astype(F32)
        total_out[...] = grown.astype(BF16)
        for dx, copy in total_copies.items():
            pl.when(at_x + dx < rows_x)(copy.start)
        ahead[...] = jnp.zeros_like(ahead)
        for x in range(1, rows_x):

            @pl.when(at_x == x)
            def _():
                landed(row_in.at[0:x], row_recv.at[0])
                for i in range(x):
                    sums[Z + i : Z + i + 1, :] = row_in[i]
                row_spans[...] = jnp.exp(sums[...].T)
                landed(total_in.at[0:x], total_recv.at[0])
                gone = total_in[0].astype(F32)
                for i in range(1, x):
                    gone = factor(row_spans, Z + i) * gone + total_in[i].astype(F32)
                ahead[...] = gone

        entry = ahead[...]
        for z in range(Z):
            enter_out[z] = entry.astype(BF16)
            if z < Z - 1:
                entry = factor(spans, z) * entry + tile_in[z].astype(F32)
        for z in range(EARLY):
            pl.when(at_z != z)(enter_copies[z].start)
        for z, copy in zip(far_first, enter_copies[EARLY:]):
            pl.when(z >= EARLY)(copy.start)
        enter_in[at_z] = enter_out[at_z]
        landed(enter_in.at[0 : Z - 1], enter_recv.at[0])
        pass_copy.start()
        for z in range(Z):
            part = part_of(z)
            carry[z] = (
                wide(decay[0, part, :]) * enter_in[z].astype(F32) + core_in[part, :].astype(F32)
            ).astype(BF16)

    @pl.when(feeds)
    def _():
        for j, hand in zip((1, 0), hand_copies):
            landed(w_near.at[j], w_recv.at[j])
            hand.start()
        pass_copy.wait_recv()

    carried = carry[...].reshape(DK, DV)

    split = pieces // 2
    order = [i + j * split for i in range(split) for j in range(2)]
    parts = [slice(i * TOKENS, (i + 1) * TOKENS) for i in range(pieces)]
    g_copies = [
        remote(
            gated.at[0, parts[i], :], gated.at[1, parts[i], :], g_send.at[0], g_recv.at[i],
            near_a if i < split else near_b,
        )
        for i in range(pieces)
    ]
    y_copies = [
        remote(
            y_out.at[parts[i], :], y_in.at[parts[i], :], y_send.at[0], y_recv.at[i // 2],
            near_b if i < split else near_a,
        )
        for i in range(pieces)
    ]
    for i in order:
        part = parts[i]
        a = att[part, :] + dot(qg[part, :], carried)
        spread = jnp.mean(a * a, axis=-1, keepdims=True)
        gated[0, part, :] = (a * lax.rsqrt(spread + 1e-05) * act[part, :]).astype(BF16)
        g_copies[i].start()
    landed(w, w_sem.at[0])
    pl.when(scans)(lambda: landed(w_near, hand_recv.at[0]))

    for i in order:
        part = parts[i]
        g_copies[i].wait_recv()
        j = i // split
        y_out[part, :] = (
            dot(gated[0, part, :], w[2 - j]) + dot(gated[1, part, :], w_near[1, j])
        ).astype(BF16)
        y_copies[i].start()
    for i in order:
        part = parts[i]
        mine[part, :] = dot(gated[0, part, :], w[0]) + dot(gated[1, part, :], w_near[0, i // split])
    for i in [i + j * split // 2 for i in range(split // 2) for j in range(2)]:
        part = slice(2 * i * TOKENS, 2 * (i + 1) * TOKENS)
        landed(y_in.at[part, :], y_recv.at[i])
        out[part, :] = (mine[part, :] + y_in[part, :].astype(F32)).astype(BF16)

    landed(gated.at[0], g_send.at[0])
    landed(y_out, y_send.at[0])

    @pl.when(feeds)
    def _():
        log_copy.wait_send()
        landed(core_out, core_send.at[0])
        landed(w_near, w_send.at[0])
        landed(w_near, hand_send.at[0])

    @pl.when(scans)
    def _():
        landed(sum_in.at[0 : Z - 1], sum_send.at[0])
        landed(tile_out.at[0 : Z - 1], tile_send.at[0])
        landed(enter_out.at[0 : Z - 1], enter_send.at[0])
        pass_copy.wait_send()
        for x in range(rows_x - 1):

            @pl.when(at_x == x)
            def _():
                landed(row_in.at[0 : rows_x - 1 - x], row_send.at[0])
                landed(total_in.at[0 : rows_x - 1 - x], total_send.at[0])


def shards(n_seq, n_head, queries, key_vectors, values, log_gate, out_gate, norm_gain, out_weight):
    length = queries.shape[0]
    width = out_weight.shape[1] // n_head
    blocks = length // SPAN
    pieces = length // TOKENS
    rows_x = n_seq // 2 // Z
    VM = pltpu.VMEM
    dma = pltpu.SemaphoreType.DMA
    tiles = VM((Z, DK // Z, DV), BF16)
    row = VM((1, DK), F32)
    scratch = [
        VM((length, DK), BF16), VM((length, DK), BF16), VM((length, DV), BF16),
        VM((length, DK), BF16), VM((length, DV), BF16), VM((1, DV), F32),
        VM((3, DV, width), BF16), VM((2, 2, DV, width), BF16),
        VM((blocks, SPAN, DK), F32), VM((blocks, DK), F32), VM((length, DK), BF16),
        VM((length, DK), BF16), VM((length, DV), F32), VM((length, DV), F32), VM((DK, DV), F32),
        row, row, VM((DK, DV), F32), VM((DK, DV), BF16), VM((DK, DV), BF16), VM((2, DK, 128), F32),
        row, VM((Z, 1, DK), F32), row, VM((rows_x, 1, DK), F32),
        VM((128, DK), F32), VM((DK, 128), F32), VM((DK, 128), F32),
        tiles, tiles, VM((DK // Z, DV), BF16), VM((rows_x, DK // Z, DV), BF16),
        VM((DK // Z, DV), F32), tiles, tiles, tiles,
        VM((2, length, DV), BF16), VM((length, width), F32),
        VM((length, width), BF16), VM((length, width), BF16),
        dma((6,)), dma((1,)), dma((1,)), dma((2,)), dma((1,)), dma((1,)),
        dma((1,)), dma((1,)), dma((1,)), dma((2,)),
        dma((1,)), dma((1,)), dma((1,)), dma((1,)), dma((1,)), dma((1,)),
        dma((1,)), dma((1,)), dma((1,)), dma((1,)), dma((1,)), dma((1,)),
        dma((1,)), dma((pieces,)), dma((1,)), dma((pieces // 2,)),
    ]
    return pl.pallas_call(
        functools.partial(kernel, n_seq, n_head),
        out_shape=pltpu.VMEM((length, width), BF16),
        in_specs=[pl.BlockSpec(memory_space=pl.ANY)] * 7,
        out_specs=pl.BlockSpec(memory_space=pltpu.VMEM),
        scratch_shapes=scratch,
        compiler_params=pltpu.CompilerParams(
            collective_id=0, has_side_effects=True, vmem_limit_bytes=56 * 2**20
        ),
        name="gated_layer",
    )(queries, key_vectors, values, log_gate, out_gate, norm_gain.reshape(1, DV), out_weight)


def solution(mesh):
    in_specs = (
        P("seq", "head"),
        P("seq", "head"),
        P("seq", "head"),
        P("seq", "head"),
        P("seq", "head"),
        P("head"),
        P("head", None),
    )
    out_specs = P("seq", "head")
    body = functools.partial(shards, mesh.shape["seq"], mesh.shape["head"])
    return jax.shard_map(body, mesh=mesh, in_specs=in_specs, out_specs=out_specs, check_vma=False)
```

```python
import functools

import jax
import jax.numpy as jnp
from jax import lax
from jax.experimental import pallas as pl
from jax.experimental.pallas import tpu as pltpu
from jax.sharding import PartitionSpec as P

DK = 256
DV = 512
SPAN = 64
TOKENS = 64
Z = 8
EARLY = 3
F32 = jnp.float32
BF16 = jnp.bfloat16
MESH = pl.DeviceIdType.MESH


def dot(a, b, dims=((1,), (0,))):
    return lax.dot_general(a, b, (dims, ((), ())), preferred_element_type=F32)


def kernel(
    n_seq, n_head,
    q_hbm, k_hbm, v_hbm, g_hbm, o_hbm, gain_hbm, w_hbm,
    out,
    q, k, v, g, o, gain, w, w_near,
    run, ends, kd, qg, att, act, state,
    log_out, log_in, own_state, core_out, core_in, decay,
    sum_out, sum_in, row_out, row_in, sums, spans, row_spans,
    tile_out, tile_in, total_out, total_in, ahead, enter_out, enter_in, fac, lead,
    gated, mine, y_out, y_in,
    load_sem, w_sem, w_send, w_recv, hand_send, hand_recv,
    log_send, log_recv, core_send, core_recv,
    sum_send, sum_recv, row_send, row_recv, tile_send, tile_recv,
    total_send, total_recv, enter_send, enter_recv, pass_send, pass_recv,
    g_send, g_recv, y_send, y_recv,
):
    loads = [
        pltpu.make_async_copy(src, dst, load_sem.at[i])
        for i, (src, dst) in enumerate(
            ((g_hbm, g), (k_hbm, k), (v_hbm, v), (q_hbm, q), (o_hbm, o), (gain_hbm, gain))
        )
    ]
    for load in loads[:3]:
        load.start()
    length = q.shape[0]
    blocks = length // SPAN
    pieces = length // TOKENS
    width = w_hbm.shape[1] // n_head
    rows_x = n_seq // 2 // Z
    part_rows = DK // Z
    copies = DV // 128
    seq = lax.axis_index("seq")
    head = lax.axis_index("head")
    core = lax.rem(seq, 2)
    chip = lax.div(seq, 2)
    feeds = core == 0
    scans = core == 1
    at_x = lax.div(chip, Z)
    at_z = lax.rem(chip, Z)
    head_a = head + 1 - 2 * lax.rem(head, 2)
    head_b = n_head - 1 - head
    head_c = n_head - 1 - head_a
    sibling = {"seq": seq + 1 - 2 * core, "head": head}
    near_a = {"seq": seq, "head": head_a}
    near_b = {"seq": seq, "head": head_b}

    def mate(x, z):
        return {"seq": (x * Z + z) * 2 + core, "head": head}

    in_row = [mate(at_x, lax.rem(at_z + dz, Z)) for dz in range(1, Z)]
    later = {dx: mate(lax.rem(at_x + dx, rows_x), at_z) for dx in (2, 1, 3)}

    def columns(which):
        return pl.ds(pl.multiple_of(which * width, 128), width)

    def remote(src, dst, send, recv, device):
        return pltpu.make_async_remote_copy(
            src_ref=src, dst_ref=dst, send_sem=send, recv_sem=recv,
            device_id=device, device_id_type=MESH,
        )

    def landed(ref, sem):
        pltpu.make_async_copy(ref, ref, sem).wait()

    barrier = pltpu.get_barrier_semaphore()

    def greet(friends):
        for friend in friends:
            pl.semaphore_signal(barrier, inc=1, device_id=friend, device_id_type=MESH)

    near = [sibling, near_a, near_b]
    greet(near)
    pl.when(scans)(lambda: greet(in_row + list(later.values())))
    w_loads = [
        pltpu.make_async_copy(w_hbm.at[:, columns(which)], w.at[j], w_sem.at[0])
        for j, which in enumerate((head, head_a, head_b))
    ]
    w_copies = [
        remote(w_hbm.at[:, columns(which)], w_near.at[j, i], w_send.at[0], w_recv.at[j], device)
        for which, j, i, device in (
            (head_c, 1, 0, near_a), (head_c, 1, 1, near_b),
            (head_a, 0, 0, near_a), (head_b, 0, 1, near_b),
        )
    ]
    hand_copies = [
        remote(w_near.at[j], w_near.at[j], hand_send.at[0], hand_recv.at[0], sibling) for j in (1, 0)
    ]
    log_copy = remote(log_out, log_in, log_send.at[0], log_recv.at[0], sibling)
    channels = [slice(0, DK // 2), slice(DK // 2, DK)]
    core_copies = [
        remote(core_out.at[cols, :], core_in.at[cols, :], core_send.at[0], core_recv.at[i], sibling)
        for i, cols in enumerate(channels)
    ]

    tri = (
        lax.broadcasted_iota(jnp.int32, (SPAN, SPAN), 0)
        >= lax.broadcasted_iota(jnp.int32, (SPAN, SPAN), 1)
    )
    ones = jnp.where(tri, 1.0, 0.0).astype(BF16)
    loads[0].wait()
    total = jnp.zeros((1, DK), F32)
    endings = []
    for b in range(blocks):
        r = dot(ones, g[b * SPAN : (b + 1) * SPAN, :])
        run[b] = r
        endings.append(r[SPAN - 1 : SPAN, :])
        ends[b : b + 1, :] = total
        total = total + endings[b]
    log_out[...] = total
    loads[1].wait()
    tail = jnp.zeros((1, DK), F32)
    for b in reversed(range(blocks)):
        part = slice(b * SPAN, (b + 1) * SPAN)
        kd[part, :] = (k[part, :].astype(F32) * jnp.exp((endings[b] - run[b]) + tail)).astype(BF16)
        tail = tail + endings[b]
    loads[2].wait()

    @pl.when(feeds)
    def _():
        pl.semaphore_wait(barrier, len(near))
        log_copy.start()

    for cols, core_copy in zip(channels, core_copies):
        grown = dot(kd[:, cols], v[...], ((0,), (0,)))
        own_state[cols, :] = grown
        core_out[cols, :] = grown.astype(BF16)
        pl.when(feeds)(core_copy.start)
    for load in loads[3:] + w_loads:
        load.start()

    @pl.when(feeds)
    def _():
        for copy in w_copies:
            copy.start()

    def lanes(row):
        return jnp.broadcast_to(row, (128, DK)).T

    def wide(columns):
        return jnp.concatenate([columns] * copies, axis=1)

    def part_of(z):
        return slice(z * part_rows, (z + 1) * part_rows)

    sum_copies = [
        remote(sum_out, sum_in.at[at_z], sum_send.at[0], sum_recv.at[0], device)
        for device in in_row
    ]
    far_first = [lax.rem(at_z + dz, Z) for dz in (4, 3, 5, 2, 6, 1, 7)]
    tile_copies = [
        remote(tile_out.at[z], tile_in.at[at_z], tile_send.at[0], tile_recv.at[0], mate(at_x, z))
        for z in far_first
    ]
    row_copies = {
        dx: remote(row_out, row_in.at[at_x], row_send.at[0], row_recv.at[0], device)
        for dx, device in later.items()
    }
    total_copies = {
        dx: remote(total_out, total_in.at[at_x], total_send.at[0], total_recv.at[0], device)
        for dx, device in later.items()
    }
    enter_copies = [
        remote(enter_out.at[z], enter_in.at[at_z], enter_send.at[0], enter_recv.at[0], mate(at_x, z))
        for z in list(range(EARLY)) + far_first
    ]
    pass_copy = remote(enter_in, enter_in, pass_send.at[0], pass_recv.at[0], sibling)

    @pl.when(scans)
    def _():
        log_copy.wait_recv()
        sum_out[...] = log_out[...] + log_in[...]
        decay[...] = lanes(jnp.exp(log_out[...]))
        sum_in[at_z] = sum_out[...]
        pl.semaphore_wait(barrier, len(near) + len(in_row) + len(later))
        for copy in sum_copies:
            copy.start()
        for i, core_copy in enumerate(core_copies):
            core_copy.wait_recv()
            for z in range(i * Z // 2, (i + 1) * Z // 2):
                part = part_of(z)
                tile_out[z] = (
                    wide(decay[part, :]) * core_in[part, :].astype(F32) + own_state[part, :]
                ).astype(BF16)
        for copy in tile_copies:
            copy.start()
        tile_in[at_z] = tile_out[at_z]

    for load in loads[3:]:
        load.wait()

    @pl.when(feeds)
    def _():
        state[...] = jnp.zeros_like(state)
        lead[...] = jnp.zeros_like(lead)

    @pl.when(scans)
    def _():
        state[...] = core_in[...].astype(F32)
        lead[...] = log_in[...]


    def local(b, _):
        part = pl.ds(pl.multiple_of(b * SPAN, SPAN), SPAN)
        r = run[b]
        middle = r[SPAN // 2 : SPAN // 2 + 1, :]
        ending = r[SPAN - 1 : SPAN, :]
        before = ends[pl.ds(b, 1), :] + lead[...]
        qf = q[part, :].astype(F32)
        kf = k[part, :].astype(F32)
        qi = qf * jnp.exp(r)
        qg[part, :] = (qi * jnp.exp(before)).astype(BF16)
        q_intra = (qf * jnp.exp(r - middle)).astype(BF16)
        k_intra = (kf * jnp.exp(middle - r)).astype(BF16)
        k_state = (kf * jnp.exp(ending - r)).astype(BF16)
        vb = v[part, :]
        scores = dot(q_intra, k_intra, ((1,), (1,)))
        weights = jnp.where(tri, scores, 0.0).astype(BF16)
        held = state[...]
        att[part, :] = dot(weights, vb) + dot(qi.astype(BF16), held.astype(BF16))
        state[...] = held * wide(lanes(jnp.exp(ending))) + dot(k_state, vb, ((0,), (0,)))
        of = o[part, :].astype(F32)
        act[part, :] = of / (1.0 + jnp.exp(-of)) * gain[...]
        return 0

    lax.fori_loop(0, blocks, local, 0)

    @pl.when(scans)
    def _():
        sums[...] = jnp.zeros_like(sums)
        landed(sum_in.at[0 : Z - 1], sum_recv.at[0])
        along = jnp.zeros((1, DK), F32)
        for z in range(Z):
            sums[z : z + 1, :] = sum_in[z]
            along = along + sum_in[z]
        row_out[...] = along
        for dx, copy in row_copies.items():
            pl.when(at_x + dx < rows_x)(copy.start)
        spans[...] = jnp.exp(sums[...].T)
        own_rows = pl.ds(pl.multiple_of(at_z * part_rows, part_rows), part_rows)

        def spread(table, i):
            fac[i] = jnp.broadcast_to(table[own_rows, :][:, i : i + 1], (part_rows, 128))

        for z in range(Z):
            spread(spans, z)
        landed(tile_in.at[0 : Z - 1], tile_recv.at[0])
        grown = tile_in[0].astype(F32)
        for z in range(1, Z):
            grown = wide(fac[z]) * grown + tile_in[z].astype(F32)
        total_out[...] = grown.astype(BF16)
        for dx, copy in total_copies.items():
            pl.when(at_x + dx < rows_x)(copy.start)
        ahead[...] = jnp.zeros_like(ahead)
        for x in range(1, rows_x):

            @pl.when(at_x == x)
            def _():
                landed(row_in.at[0:x], row_recv.at[0])
                for i in range(x):
                    sums[Z + i : Z + i + 1, :] = row_in[i]
                row_spans[...] = jnp.exp(sums[...].T)
                for i in range(1, x):
                    spread(row_spans, Z + i)
                landed(total_in.at[0:x], total_recv.at[0])
                gone = total_in[0].astype(F32)
                for i in range(1, x):
                    gone = wide(fac[Z + i]) * gone + total_in[i].astype(F32)
                ahead[...] = gone

        entry = ahead[...]
        for z in range(Z):
            enter_out[z] = entry.astype(BF16)
            if z < EARLY:
                pl.when(at_z != z)(enter_copies[z].start)
            if z < Z - 1:
                entry = wide(fac[z]) * entry + tile_in[z].astype(F32)
        for z, copy in zip(far_first, enter_copies[EARLY:]):
            pl.when(z >= EARLY)(copy.start)
        enter_in[at_z] = enter_out[at_z]
        landed(enter_in.at[0 : Z - 1], enter_recv.at[0])
        pass_copy.start()

    @pl.when(feeds)
    def _():
        for j, hand in zip((1, 0), hand_copies):
            landed(w_near.at[j], w_recv.at[j])
            hand.start()
        pass_copy.wait_recv()

    carried = enter_in[...].reshape(DK, DV)

    split = pieces // 2
    order = [i + j * split for i in range(split) for j in range(2)]
    parts = [slice(i * TOKENS, (i + 1) * TOKENS) for i in range(pieces)]
    g_copies = [
        remote(
            gated.at[0, parts[i], :], gated.at[1, parts[i], :], g_send.at[0], g_recv.at[i],
            near_a if i < split else near_b,
        )
        for i in range(pieces)
    ]
    y_copies = [
        remote(
            y_out.at[parts[i], :], y_in.at[parts[i], :], y_send.at[0], y_recv.at[i // 2],
            near_b if i < split else near_a,
        )
        for i in range(pieces)
    ]
    for i in order:
        part = parts[i]
        a = att[part, :] + dot(qg[part, :], carried)
        spread = jnp.mean(a * a, axis=-1, keepdims=True)
        gated[0, part, :] = (a * lax.rsqrt(spread + 1e-05) * act[part, :]).astype(BF16)
        g_copies[i].start()
    landed(w, w_sem.at[0])
    pl.when(scans)(lambda: landed(w_near, hand_recv.at[0]))

    for i in order:
        part = parts[i]
        g_copies[i].wait_recv()
        j = i // split
        y_out[part, :] = (
            dot(gated[0, part, :], w[2 - j]) + dot(gated[1, part, :], w_near[1, j])
        ).astype(BF16)
        y_copies[i].start()
    for i in order:
        part = parts[i]
        mine[part, :] = dot(gated[0, part, :], w[0]) + dot(gated[1, part, :], w_near[0, i // split])
    for i in [i + j * split // 2 for i in range(split // 2) for j in range(2)]:
        part = slice(2 * i * TOKENS, 2 * (i + 1) * TOKENS)
        landed(y_in.at[part, :], y_recv.at[i])
        out[part, :] = (mine[part, :] + y_in[part, :].astype(F32)).astype(BF16)

    landed(gated.at[0], g_send.at[0])
    landed(y_out, y_send.at[0])

    @pl.when(feeds)
    def _():
        log_copy.wait_send()
        landed(core_out, core_send.at[0])
        landed(w_near, w_send.at[0])
        landed(w_near, hand_send.at[0])

    @pl.when(scans)
    def _():
        landed(sum_in.at[0 : Z - 1], sum_send.at[0])
        landed(tile_out.at[0 : Z - 1], tile_send.at[0])
        landed(enter_out.at[0 : Z - 1], enter_send.at[0])
        pass_copy.wait_send()
        for x in range(rows_x - 1):

            @pl.when(at_x == x)
            def _():
                landed(row_in.at[0 : rows_x - 1 - x], row_send.at[0])
                landed(total_in.at[0 : rows_x - 1 - x], total_send.at[0])


def shards(n_seq, n_head, queries, key_vectors, values, log_gate, out_gate, norm_gain, out_weight):
    length = queries.shape[0]
    width = out_weight.shape[1] // n_head
    blocks = length // SPAN
    pieces = length // TOKENS
    rows_x = n_seq // 2 // Z
    VM = pltpu.VMEM
    dma = pltpu.SemaphoreType.DMA
    tiles = VM((Z, DK // Z, DV), BF16)
    row = VM((1, DK), F32)
    scratch = [
        VM((length, DK), BF16), VM((length, DK), BF16), VM((length, DV), BF16),
        VM((length, DK), BF16), VM((length, DV), BF16), VM((1, DV), F32),
        VM((3, DV, width), BF16), VM((2, 2, DV, width), BF16),
        VM((blocks, SPAN, DK), F32), VM((blocks, DK), F32), VM((length, DK), BF16),
        VM((length, DK), BF16), VM((length, DV), F32), VM((length, DV), F32), VM((DK, DV), F32),
        row, row, VM((DK, DV), F32), VM((DK, DV), BF16), VM((DK, DV), BF16), VM((DK, 128), F32),
        row, VM((Z, 1, DK), F32), row, VM((rows_x, 1, DK), F32),
        VM((128, DK), F32), VM((DK, 128), F32), VM((DK, 128), F32),
        tiles, tiles, VM((DK // Z, DV), BF16), VM((rows_x, DK // Z, DV), BF16),
        VM((DK // Z, DV), F32), tiles, tiles, VM((Z + rows_x, DK // Z, 128), F32), row,
        VM((2, length, DV), BF16), VM((length, width), F32),
        VM((length, width), BF16), VM((length, width), BF16),
        dma((6,)), dma((1,)), dma((1,)), dma((2,)), dma((1,)), dma((1,)),
        dma((1,)), dma((1,)), dma((1,)), dma((2,)),
        dma((1,)), dma((1,)), dma((1,)), dma((1,)), dma((1,)), dma((1,)),
        dma((1,)), dma((1,)), dma((1,)), dma((1,)), dma((1,)), dma((1,)),
        dma((1,)), dma((pieces,)), dma((1,)), dma((pieces // 2,)),
    ]
    return pl.pallas_call(
        functools.partial(kernel, n_seq, n_head),
        out_shape=pltpu.VMEM((length, width), BF16),
        in_specs=[pl.BlockSpec(memory_space=pl.ANY)] * 7,
        out_specs=pl.BlockSpec(memory_space=pltpu.VMEM),
        scratch_shapes=scratch,
        compiler_params=pltpu.CompilerParams(
            collective_id=0, has_side_effects=True, vmem_limit_bytes=56 * 2**20
        ),
        name="gated_layer",
    )(queries, key_vectors, values, log_gate, out_gate, norm_gain.reshape(1, DV), out_weight)


def solution(mesh):
    in_specs = (
        P("seq", "head"),
        P("seq", "head"),
        P("seq", "head"),
        P("seq", "head"),
        P("seq", "head"),
        P("head"),
        P("head", None),
    )
    out_specs = P("seq", "head")
    body = functools.partial(shards, mesh.shape["seq"], mesh.shape["head"])
    return jax.shard_map(body, mesh=mesh, in_specs=in_specs, out_specs=out_specs, check_vma=False)
```

```python
import functools

import jax
import jax.numpy as jnp
from jax import lax
from jax.experimental import pallas as pl
from jax.experimental.pallas import tpu as pltpu
from jax.sharding import PartitionSpec as P

DK = 256
DV = 512
SPAN = 64
TOKENS = 64
Z = 8
EARLY = 3
F32 = jnp.float32
BF16 = jnp.bfloat16
MESH = pl.DeviceIdType.MESH


def dot(a, b, dims=((1,), (0,))):
    return lax.dot_general(a, b, (dims, ((), ())), preferred_element_type=F32)


def kernel(
    n_seq, n_head,
    q_hbm, k_hbm, v_hbm, g_hbm, o_hbm, gain_hbm, w_hbm,
    out,
    q, k, v, g, o, gain, w, w_near,
    run, ends, kd, qg, att, act, state,
    log_out, log_in, own_state, core_out, core_in, decay,
    sum_out, sum_in, row_out, row_in, sums, spans, row_spans,
    tile_out, tile_in, total_out, total_in, ahead, enter_out, enter_in, fac, lead,
    gated, mine, y_out, y_in,
    load_sem, w_sem, hand_sem, log_sem, core_sem, pass_sem,
    sum_send, sum_recv, row_send, row_recv, tile_send, tile_recv,
    total_send, total_recv, enter_send, enter_recv,
    g_recv, y_send, y_recv,
):
    loads = [
        pltpu.make_async_copy(src, dst, load_sem.at[i])
        for i, (src, dst) in enumerate(
            ((g_hbm, g), (k_hbm, k), (v_hbm, v), (q_hbm, q), (o_hbm, o), (gain_hbm, gain))
        )
    ]
    for load in loads[:3]:
        load.start()
    length = q.shape[0]
    blocks = length // SPAN
    pieces = length // TOKENS
    width = w_hbm.shape[1] // n_head
    rows_x = n_seq // 2 // Z
    part_rows = DK // Z
    copies = DV // 128
    seq = lax.axis_index("seq")
    head = lax.axis_index("head")
    core = lax.rem(seq, 2)
    chip = lax.div(seq, 2)
    feeds = core == 0
    scans = core == 1
    at_x = lax.div(chip, Z)
    at_z = lax.rem(chip, Z)
    head_a = head + 1 - 2 * lax.rem(head, 2)
    head_b = n_head - 1 - head
    head_c = n_head - 1 - head_a
    sibling = {"seq": seq + 1 - 2 * core, "head": head}
    near_a = {"seq": seq, "head": head_a}
    near_b = {"seq": seq, "head": head_b}

    def mate(x, z):
        return {"seq": (x * Z + z) * 2 + core, "head": head}

    in_row = [mate(at_x, lax.rem(at_z + dz, Z)) for dz in range(1, Z)]
    later = {dx: mate(lax.rem(at_x + dx, rows_x), at_z) for dx in (2, 1, 3)}

    def columns(which):
        return pl.ds(pl.multiple_of(which * width, 128), width)

    def remote(src, dst, send, recv, device):
        return pltpu.make_async_remote_copy(
            src_ref=src, dst_ref=dst, send_sem=send, recv_sem=recv,
            device_id=device, device_id_type=MESH,
        )

    def landed(ref, sem):
        pltpu.make_async_copy(ref, ref, sem).wait()

    barrier = pltpu.get_barrier_semaphore()

    def greet(friends):
        for friend in friends:
            pl.semaphore_signal(barrier, inc=1, device_id=friend, device_id_type=MESH)

    near = [sibling, near_a, near_b]
    greet(near)
    pl.when(scans)(lambda: greet(in_row + list(later.values())))
    w_loads = [
        pltpu.make_async_copy(w_hbm.at[:, columns(which)], w.at[j], w_sem.at[0])
        for j, which in enumerate((head, head_a, head_b))
    ]
    w_copies = [
        remote(w_hbm.at[:, columns(which)], w_near.at[j, i], sum_send.at[0], (sum_recv, tile_recv)[j].at[0], device)
        for which, j, i, device in (
            (head_c, 1, 0, near_a), (head_c, 1, 1, near_b),
            (head_a, 0, 0, near_a), (head_b, 0, 1, near_b),
        )
    ]
    hand_copies = [
        remote(w_near.at[j], w_near.at[j], hand_sem.at[0], hand_sem.at[0], sibling) for j in (1, 0)
    ]
    log_copy = remote(log_out, log_in, log_sem.at[0], log_sem.at[0], sibling)
    core_copy = remote(core_out, core_in, core_sem.at[0], core_sem.at[0], sibling)

    tri = (
        lax.broadcasted_iota(jnp.int32, (SPAN, SPAN), 0)
        >= lax.broadcasted_iota(jnp.int32, (SPAN, SPAN), 1)
    )
    ones = jnp.where(tri, 1.0, 0.0).astype(BF16)
    loads[0].wait()
    total = jnp.zeros((1, DK), F32)
    endings = []
    for b in range(blocks):
        r = dot(ones, g[b * SPAN : (b + 1) * SPAN, :])
        run[b] = r
        endings.append(r[SPAN - 1 : SPAN, :])
        ends[b : b + 1, :] = total
        total = total + endings[b]
    log_out[...] = total
    loads[1].wait()
    tail = jnp.zeros((1, DK), F32)
    for b in reversed(range(blocks)):
        part = slice(b * SPAN, (b + 1) * SPAN)
        kd[part, :] = (k[part, :].astype(F32) * jnp.exp((endings[b] - run[b]) + tail)).astype(BF16)
        tail = tail + endings[b]
    loads[2].wait()

    @pl.when(feeds)
    def _():
        pl.semaphore_wait(barrier, len(near))
        log_copy.start()

    grown = dot(kd[...], v[...], ((0,), (0,)))
    own_state[...] = grown
    core_out[...] = grown.astype(BF16)
    pl.when(feeds)(core_copy.start)
    for load in loads[3:] + w_loads:
        load.start()

    @pl.when(feeds)
    def _():
        for copy in w_copies:
            copy.start()

    def lanes(row):
        return jnp.broadcast_to(row, (128, DK)).T

    def wide(columns):
        return jnp.concatenate([columns] * copies, axis=1)

    def part_of(z):
        return slice(z * part_rows, (z + 1) * part_rows)

    sum_copies = [
        remote(sum_out, sum_in.at[at_z], sum_send.at[0], sum_recv.at[0], device)
        for device in in_row
    ]
    far_first = [lax.rem(at_z + dz, Z) for dz in (4, 3, 5, 2, 6, 1, 7)]
    tile_copies = [
        remote(tile_out.at[z], tile_in.at[at_z], tile_send.at[0], tile_recv.at[0], mate(at_x, z))
        for z in far_first
    ]
    row_copies = {
        dx: remote(row_out, row_in.at[at_x], row_send.at[0], row_recv.at[0], device)
        for dx, device in later.items()
    }
    total_copies = {
        dx: remote(total_out, total_in.at[at_x], total_send.at[0], total_recv.at[0], device)
        for dx, device in later.items()
    }
    enter_copies = [
        remote(enter_out.at[z], enter_in.at[at_z], enter_send.at[0], enter_recv.at[0], mate(at_x, z))
        for z in list(range(EARLY)) + far_first
    ]
    pass_copy = remote(enter_in, enter_in, pass_sem.at[0], pass_sem.at[0], sibling)

    @pl.when(scans)
    def _():
        log_copy.wait_recv()
        sum_out[...] = log_out[...] + log_in[...]
        decay[...] = lanes(jnp.exp(log_out[...]))
        sum_in[at_z] = sum_out[...]
        pl.semaphore_wait(barrier, len(near) + len(in_row) + len(later))
        for copy in sum_copies:
            copy.start()
        core_copy.wait_recv()
        for z in range(Z):
            part = part_of(z)
            tile_out[z] = (
                wide(decay[part, :]) * core_in[part, :].astype(F32) + own_state[part, :]
            ).astype(BF16)
        for copy in tile_copies:
            copy.start()
        tile_in[at_z] = tile_out[at_z]

    for load in loads[3:]:
        load.wait()

    @pl.when(feeds)
    def _():
        state[...] = jnp.zeros_like(state)
        lead[...] = jnp.zeros_like(lead)

    @pl.when(scans)
    def _():
        state[...] = core_in[...].astype(F32)
        lead[...] = log_in[...]


    def local(b, _):
        part = pl.ds(pl.multiple_of(b * SPAN, SPAN), SPAN)
        r = run[b]
        middle = r[SPAN // 2 : SPAN // 2 + 1, :]
        ending = r[SPAN - 1 : SPAN, :]
        before = ends[pl.ds(b, 1), :] + lead[...]
        qf = q[part, :].astype(F32)
        kf = k[part, :].astype(F32)
        qi = qf * jnp.exp(r)
        qg[part, :] = (qi * jnp.exp(before)).astype(BF16)
        q_intra = (qf * jnp.exp(r - middle)).astype(BF16)
        k_intra = (kf * jnp.exp(middle - r)).astype(BF16)
        k_state = (kf * jnp.exp(ending - r)).astype(BF16)
        vb = v[part, :]
        scores = dot(q_intra, k_intra, ((1,), (1,)))
        weights = jnp.where(tri, scores, 0.0).astype(BF16)
        held = state[...]
        att[part, :] = dot(weights, vb) + dot(qi.astype(BF16), held.astype(BF16))
        state[...] = held * wide(lanes(jnp.exp(ending))) + dot(k_state, vb, ((0,), (0,)))
        of = o[part, :].astype(F32)
        act[part, :] = of / (1.0 + jnp.exp(-of)) * gain[...]
        return 0

    lax.fori_loop(0, blocks, local, 0)

    @pl.when(scans)
    def _():
        sums[...] = jnp.zeros_like(sums)
        landed(sum_in.at[0 : Z - 1], sum_recv.at[0])
        along = jnp.zeros((1, DK), F32)
        for z in range(Z):
            sums[z : z + 1, :] = sum_in[z]
            along = along + sum_in[z]
        row_out[...] = along
        for dx, copy in row_copies.items():
            pl.when(at_x + dx < rows_x)(copy.start)
        spans[...] = jnp.exp(sums[...].T)
        own_rows = pl.ds(pl.multiple_of(at_z * part_rows, part_rows), part_rows)

        def spread(table, i):
            fac[i] = jnp.broadcast_to(table[own_rows, :][:, i : i + 1], (part_rows, 128))

        for z in range(Z):
            spread(spans, z)
        landed(tile_in.at[0 : Z - 1], tile_recv.at[0])
        grown = tile_in[0].astype(F32)
        for z in range(1, Z):
            grown = wide(fac[z]) * grown + tile_in[z].astype(F32)
        total_out[...] = grown.astype(BF16)
        for dx, copy in total_copies.items():
            pl.when(at_x + dx < rows_x)(copy.start)
        ahead[...] = jnp.zeros_like(ahead)
        for x in range(1, rows_x):

            @pl.when(at_x == x)
            def _():
                landed(row_in.at[0:x], row_recv.at[0])
                for i in range(x):
                    sums[Z + i : Z + i + 1, :] = row_in[i]
                row_spans[...] = jnp.exp(sums[...].T)
                for i in range(1, x):
                    spread(row_spans, Z + i)
                landed(total_in.at[0:x], total_recv.at[0])
                gone = total_in[0].astype(F32)
                for i in range(1, x):
                    gone = wide(fac[Z + i]) * gone + total_in[i].astype(F32)
                ahead[...] = gone

        entry = ahead[...]
        for z in range(Z):
            enter_out[z] = entry.astype(BF16)
            if z < EARLY:
                pl.when(at_z != z)(enter_copies[z].start)
            if z < Z - 1:
                entry = wide(fac[z]) * entry + tile_in[z].astype(F32)
        for z, copy in zip(far_first, enter_copies[EARLY:]):
            pl.when(z >= EARLY)(copy.start)
        enter_in[at_z] = enter_out[at_z]
        landed(enter_in.at[0 : Z - 1], enter_recv.at[0])
        pass_copy.start()

    @pl.when(feeds)
    def _():
        for j, hand in zip((1, 0), hand_copies):
            landed(w_near.at[j], (sum_recv, tile_recv)[j].at[0])
            hand.start()
        pass_copy.wait_recv()

    carried = enter_in[...].reshape(DK, DV)

    split = pieces // 2
    order = [i + j * split for i in range(split) for j in range(2)]
    parts = [slice(i * TOKENS, (i + 1) * TOKENS) for i in range(pieces)]
    g_copies = [
        remote(
            gated.at[0, parts[i], :], gated.at[1, parts[i], :], y_send.at[0], g_recv.at[i],
            near_a if i < split else near_b,
        )
        for i in range(pieces)
    ]
    y_copies = [
        remote(
            y_out.at[parts[i], :], y_in.at[parts[i], :], y_send.at[0], y_recv.at[i // 4],
            near_b if i < split else near_a,
        )
        for i in range(pieces)
    ]
    for i in order:
        part = parts[i]
        a = att[part, :] + dot(qg[part, :], carried)
        spread = jnp.mean(a * a, axis=-1, keepdims=True)
        gated[0, part, :] = (a * lax.rsqrt(spread + 1e-05) * act[part, :]).astype(BF16)
        g_copies[i].start()
    landed(w, w_sem.at[0])
    pl.when(scans)(lambda: landed(w_near, hand_sem.at[0]))

    for i in order:
        part = parts[i]
        g_copies[i].wait_recv()
        j = i // split
        y_out[part, :] = (
            dot(gated[0, part, :], w[2 - j]) + dot(gated[1, part, :], w_near[1, j])
        ).astype(BF16)
        y_copies[i].start()
    for i in order:
        part = parts[i]
        mine[part, :] = dot(gated[0, part, :], w[0]) + dot(gated[1, part, :], w_near[0, i // split])
    for i in range(2):
        part = slice(i * split * TOKENS, (i + 1) * split * TOKENS)
        landed(y_in.at[part, :], y_recv.at[i])
        out[part, :] = (mine[part, :] + y_in[part, :].astype(F32)).astype(BF16)

    landed(gated, y_send.at[0])

    @pl.when(feeds)
    def _():
        log_copy.wait_send()
        core_copy.wait_send()
        landed(w_near, sum_send.at[0])
        landed(w_near, hand_sem.at[0])

    @pl.when(scans)
    def _():
        landed(sum_in.at[0 : Z - 1], sum_send.at[0])
        landed(tile_out.at[0 : Z - 1], tile_send.at[0])
        landed(enter_out.at[0 : Z - 1], enter_send.at[0])
        pass_copy.wait_send()
        for x in range(rows_x - 1):

            @pl.when(at_x == x)
            def _():
                landed(row_in.at[0 : rows_x - 1 - x], row_send.at[0])
                landed(total_in.at[0 : rows_x - 1 - x], total_send.at[0])


def shards(n_seq, n_head, queries, key_vectors, values, log_gate, out_gate, norm_gain, out_weight):
    length = queries.shape[0]
    width = out_weight.shape[1] // n_head
    blocks = length // SPAN
    pieces = length // TOKENS
    rows_x = n_seq // 2 // Z
    VM = pltpu.VMEM
    dma = pltpu.SemaphoreType.DMA
    tiles = VM((Z, DK // Z, DV), BF16)
    row = VM((1, DK), F32)
    scratch = [
        VM((length, DK), BF16), VM((length, DK), BF16), VM((length, DV), BF16),
        VM((length, DK), BF16), VM((length, DV), BF16), VM((1, DV), F32),
        VM((3, DV, width), BF16), VM((2, 2, DV, width), BF16),
        VM((blocks, SPAN, DK), F32), VM((blocks, DK), F32), VM((length, DK), BF16),
        VM((length, DK), BF16), VM((length, DV), F32), VM((length, DV), F32), VM((DK, DV), F32),
        row, row, VM((DK, DV), F32), VM((DK, DV), BF16), VM((DK, DV), BF16), VM((DK, 128), F32),
        row, VM((Z, 1, DK), F32), row, VM((rows_x, 1, DK), F32),
        VM((128, DK), F32), VM((DK, 128), F32), VM((DK, 128), F32),
        tiles, tiles, VM((DK // Z, DV), BF16), VM((rows_x, DK // Z, DV), BF16),
        VM((DK // Z, DV), F32), tiles, tiles, VM((Z + rows_x, DK // Z, 128), F32), row,
        VM((2, length, DV), BF16), VM((length, width), F32),
        VM((length, width), BF16), VM((length, width), BF16),
        dma((6,)), dma((1,)), dma((1,)), dma((1,)), dma((1,)), dma((1,)),
        dma((1,)), dma((1,)), dma((1,)), dma((1,)), dma((1,)), dma((1,)),
        dma((1,)), dma((1,)), dma((1,)), dma((1,)),
        dma((pieces,)), dma((1,)), dma((pieces // 4,)),
    ]
    return pl.pallas_call(
        functools.partial(kernel, n_seq, n_head),
        out_shape=pltpu.VMEM((length, width), BF16),
        in_specs=[pl.BlockSpec(memory_space=pl.ANY)] * 7,
        out_specs=pl.BlockSpec(memory_space=pltpu.VMEM),
        scratch_shapes=scratch,
        compiler_params=pltpu.CompilerParams(
            collective_id=0, has_side_effects=True, vmem_limit_bytes=56 * 2**20
        ),
        name="gated_layer",
    )(queries, key_vectors, values, log_gate, out_gate, norm_gain.reshape(1, DV), out_weight)


def solution(mesh):
    in_specs = (
        P("seq", "head"),
        P("seq", "head"),
        P("seq", "head"),
        P("seq", "head"),
        P("seq", "head"),
        P("head"),
        P("head", None),
    )
    out_specs = P("seq", "head")
    body = functools.partial(shards, mesh.shape["seq"], mesh.shape["head"])
    return jax.shard_map(body, mesh=mesh, in_specs=in_specs, out_specs=out_specs, check_vma=False)
```

```python
import functools

import jax
import jax.numpy as jnp
from jax import lax
from jax.experimental import pallas as pl
from jax.experimental.pallas import tpu as pltpu
from jax.sharding import PartitionSpec as P

DK = 256
DV = 512
SPAN = 64
TOKENS = 64
Z = 8
EARLY = 3
F32 = jnp.float32
BF16 = jnp.bfloat16
MESH = pl.DeviceIdType.MESH


def dot(a, b, dims=((1,), (0,))):
    return lax.dot_general(a, b, (dims, ((), ())), preferred_element_type=F32)


def kernel(
    n_seq, n_head,
    q_hbm, k_hbm, v_hbm, g_hbm, o_hbm, gain_hbm, w_hbm,
    out,
    q, k, v, g, o, gain, w, w_near,
    run, ends, kd, qg, att, act, state,
    log_out, log_in, own_state, core_out, core_in, decay,
    sum_out, sum_in, row_out, row_in, sums, spans, row_spans,
    tile_out, tile_in, total_out, total_in, ahead, enter_out, enter_in, fac, lead,
    gated, mine, y_out, y_in,
    load_sem, w_sem, hand_sem, log_sem, core_sem, pass_sem,
    sum_send, sum_recv, row_send, row_recv, tile_send, tile_recv,
    total_send, total_recv, enter_send, enter_recv,
    g_recv, y_send, y_recv,
):
    loads = [
        pltpu.make_async_copy(src, dst, load_sem.at[i])
        for i, (src, dst) in enumerate(
            ((g_hbm, g), (k_hbm, k), (v_hbm, v), (q_hbm, q), (o_hbm, o), (gain_hbm, gain))
        )
    ]
    for load in loads[:3]:
        load.start()
    length = q.shape[0]
    blocks = length // SPAN
    pieces = length // TOKENS
    width = w_hbm.shape[1] // n_head
    rows_x = n_seq // 2 // Z
    part_rows = DK // Z
    copies = DV // 128
    seq = lax.axis_index("seq")
    head = lax.axis_index("head")
    core = lax.rem(seq, 2)
    chip = lax.div(seq, 2)
    feeds = core == 0
    scans = core == 1
    at_x = lax.div(chip, Z)
    at_z = lax.rem(chip, Z)
    head_a = head + 1 - 2 * lax.rem(head, 2)
    head_b = n_head - 1 - head
    head_c = n_head - 1 - head_a
    sibling = {"seq": seq + 1 - 2 * core, "head": head}
    near_a = {"seq": seq, "head": head_a}
    near_b = {"seq": seq, "head": head_b}

    def mate(x, z):
        return {"seq": (x * Z + z) * 2 + core, "head": head}

    in_row = [mate(at_x, lax.rem(at_z + dz, Z)) for dz in (4, 3, 5, 2, 6, 1, 7)]
    later = {dx: mate(lax.rem(at_x + dx, rows_x), at_z) for dx in (2, 1, 3)}

    def columns(which):
        return pl.ds(pl.multiple_of(which * width, 128), width)

    def remote(src, dst, send, recv, device):
        return pltpu.make_async_remote_copy(
            src_ref=src, dst_ref=dst, send_sem=send, recv_sem=recv,
            device_id=device, device_id_type=MESH,
        )

    def landed(ref, sem):
        pltpu.make_async_copy(ref, ref, sem).wait()

    barrier = pltpu.get_barrier_semaphore()

    def greet(friends):
        for friend in friends:
            pl.semaphore_signal(barrier, inc=1, device_id=friend, device_id_type=MESH)

    near = [sibling, near_a, near_b]
    greet(near)
    pl.when(scans)(lambda: greet(in_row + list(later.values())))
    w_loads = [
        pltpu.make_async_copy(w_hbm.at[:, columns(which)], w.at[j], w_sem.at[0])
        for j, which in enumerate((head, head_a, head_b))
    ]
    w_copies = [
        remote(w_hbm.at[:, columns(which)], w_near.at[j, i], sum_send.at[0], (sum_recv, tile_recv)[j].at[0], device)
        for which, j, i, device in (
            (head_c, 1, 0, near_a), (head_c, 1, 1, near_b),
            (head_a, 0, 0, near_a), (head_b, 0, 1, near_b),
        )
    ]
    hand_copies = [
        remote(w_near.at[j], w_near.at[j], hand_sem.at[0], hand_sem.at[0], sibling) for j in (1, 0)
    ]
    log_copy = remote(log_out, log_in, log_sem.at[0], log_sem.at[0], sibling)
    core_copy = remote(core_out, core_in, core_sem.at[0], core_sem.at[0], sibling)

    tri = (
        lax.broadcasted_iota(jnp.int32, (SPAN, SPAN), 0)
        >= lax.broadcasted_iota(jnp.int32, (SPAN, SPAN), 1)
    )
    ones = jnp.where(tri, 1.0, 0.0).astype(BF16)
    loads[0].wait()
    total = jnp.zeros((1, DK), F32)
    endings = []
    for b in range(blocks):
        r = dot(ones, g[b * SPAN : (b + 1) * SPAN, :])
        run[b] = r
        endings.append(r[SPAN - 1 : SPAN, :])
        ends[b : b + 1, :] = total
        total = total + endings[b]
    log_out[...] = total
    loads[1].wait()
    tail = jnp.zeros((1, DK), F32)
    for b in reversed(range(blocks)):
        part = slice(b * SPAN, (b + 1) * SPAN)
        kd[part, :] = (k[part, :].astype(F32) * jnp.exp((endings[b] - run[b]) + tail)).astype(BF16)
        tail = tail + endings[b]
    loads[2].wait()

    @pl.when(feeds)
    def _():
        pl.semaphore_wait(barrier, len(near))
        log_copy.start()

    grown = dot(kd[...], v[...], ((0,), (0,)))

    @pl.when(feeds)
    def _():
        core_out[...] = grown.astype(BF16)
        core_copy.start()

    @pl.when(scans)
    def _():
        own_state[...] = grown

    for load in loads[3:] + w_loads:
        load.start()

    @pl.when(feeds)
    def _():
        for copy in w_copies:
            copy.start()

    def lanes(row):
        return jnp.broadcast_to(row, (128, DK)).T

    def wide(columns):
        return jnp.concatenate([columns] * copies, axis=1)

    def part_of(z):
        return slice(z * part_rows, (z + 1) * part_rows)

    sum_copies = [
        remote(sum_out, sum_in.at[at_z], sum_send.at[0], sum_recv.at[0], device)
        for device in in_row
    ]
    far_first = [lax.rem(at_z + dz, Z) for dz in (4, 3, 5, 2, 6, 1, 7)]
    tile_copies = [
        remote(tile_out.at[z], tile_in.at[at_z], tile_send.at[0], tile_recv.at[0], mate(at_x, z))
        for z in far_first
    ]
    row_copies = {
        dx: remote(row_out, row_in.at[at_x], row_send.at[0], row_recv.at[0], device)
        for dx, device in later.items()
    }
    total_copies = {
        dx: remote(total_out, total_in.at[at_x], total_send.at[0], total_recv.at[0], device)
        for dx, device in later.items()
    }
    enter_copies = [
        remote(enter_out.at[z], enter_in.at[at_z], enter_send.at[0], enter_recv.at[0], mate(at_x, z))
        for z in list(range(EARLY)) + far_first
    ]
    pass_copy = remote(enter_in, enter_in, pass_sem.at[0], pass_sem.at[0], sibling)

    @pl.when(scans)
    def _():
        log_copy.wait_recv()
        sum_out[...] = log_out[...] + log_in[...]
        pl.semaphore_wait(barrier, len(near) + len(in_row) + len(later))
        for copy in sum_copies:
            copy.start()
        decay[...] = lanes(jnp.exp(log_out[...]))
        sum_in[at_z] = sum_out[...]
        core_copy.wait_recv()
        for z in range(Z):
            part = part_of(z)
            tile_out[z] = (
                wide(decay[part, :]) * core_in[part, :].astype(F32) + own_state[part, :]
            ).astype(BF16)
        for copy in tile_copies:
            copy.start()
        tile_in[at_z] = tile_out[at_z]

    for load in loads[3:]:
        load.wait()

    @pl.when(feeds)
    def _():
        state[...] = jnp.zeros_like(state)
        lead[...] = jnp.zeros_like(lead)

    @pl.when(scans)
    def _():
        state[...] = core_in[...].astype(F32)
        lead[...] = log_in[...]


    def local(b, _):
        part = pl.ds(pl.multiple_of(b * SPAN, SPAN), SPAN)
        r = run[b]
        middle = r[SPAN // 2 : SPAN // 2 + 1, :]
        ending = r[SPAN - 1 : SPAN, :]
        before = ends[pl.ds(b, 1), :] + lead[...]
        qf = q[part, :].astype(F32)
        kf = k[part, :].astype(F32)
        qi = qf * jnp.exp(r)
        qg[part, :] = (qi * jnp.exp(before)).astype(BF16)
        q_intra = (qf * jnp.exp(r - middle)).astype(BF16)
        k_intra = (kf * jnp.exp(middle - r)).astype(BF16)
        k_state = (kf * jnp.exp(ending - r)).astype(BF16)
        vb = v[part, :]
        scores = dot(q_intra, k_intra, ((1,), (1,)))
        weights = jnp.where(tri, scores, 0.0).astype(BF16)
        held = state[...]
        att[part, :] = dot(weights, vb) + dot(qi.astype(BF16), held.astype(BF16))
        state[...] = held * wide(lanes(jnp.exp(ending))) + dot(k_state, vb, ((0,), (0,)))
        of = o[part, :].astype(F32)
        act[part, :] = of / (1.0 + jnp.exp(-of)) * gain[...]
        return 0

    lax.fori_loop(0, blocks, local, 0)

    @pl.when(scans)
    def _():
        sums[...] = jnp.zeros_like(sums)
        landed(sum_in.at[0 : Z - 1], sum_recv.at[0])
        along = jnp.zeros((1, DK), F32)
        for z in range(Z):
            sums[z : z + 1, :] = sum_in[z]
            along = along + sum_in[z]
        row_out[...] = along
        for dx, copy in row_copies.items():
            pl.when(at_x + dx < rows_x)(copy.start)
        spans[...] = jnp.exp(sums[...].T)
        own_rows = pl.ds(pl.multiple_of(at_z * part_rows, part_rows), part_rows)

        def spread(table, i):
            fac[i] = jnp.broadcast_to(table[own_rows, :][:, i : i + 1], (part_rows, 128))

        for z in range(Z):
            spread(spans, z)
        landed(tile_in.at[0 : Z - 1], tile_recv.at[0])
        grown = tile_in[0].astype(F32)
        for z in range(1, Z):
            grown = wide(fac[z]) * grown + tile_in[z].astype(F32)
        total_out[...] = grown.astype(BF16)
        for dx, copy in total_copies.items():
            pl.when(at_x + dx < rows_x)(copy.start)
        ahead[...] = jnp.zeros_like(ahead)
        for x in range(1, rows_x):

            @pl.when(at_x == x)
            def _():
                landed(row_in.at[0:x], row_recv.at[0])
                for i in range(x):
                    sums[Z + i : Z + i + 1, :] = row_in[i]
                row_spans[...] = jnp.exp(sums[...].T)
                for i in range(1, x):
                    spread(row_spans, Z + i)
                landed(total_in.at[0:x], total_recv.at[0])
                gone = total_in[0].astype(F32)
                for i in range(1, x):
                    gone = wide(fac[Z + i]) * gone + total_in[i].astype(F32)
                ahead[...] = gone

        entry = ahead[...]
        for z in range(Z):
            enter_out[z] = entry.astype(BF16)
            if z < EARLY:
                pl.when(at_z != z)(enter_copies[z].start)
            if z < Z - 1:
                entry = wide(fac[z]) * entry + tile_in[z].astype(F32)
        for z, copy in zip(far_first, enter_copies[EARLY:]):
            pl.when(z >= EARLY)(copy.start)
        enter_in[at_z] = enter_out[at_z]
        landed(enter_in.at[0 : Z - 1], enter_recv.at[0])
        pass_copy.start()

    @pl.when(feeds)
    def _():
        for j, hand in zip((1, 0), hand_copies):
            landed(w_near.at[j], (sum_recv, tile_recv)[j].at[0])
            hand.start()
        pass_copy.wait_recv()

    carried = enter_in[...].reshape(DK, DV)

    split = pieces // 2
    order = [i + j * split for i in range(split) for j in range(2)]
    parts = [slice(i * TOKENS, (i + 1) * TOKENS) for i in range(pieces)]
    g_copies = [
        remote(
            gated.at[0, parts[i], :], gated.at[1, parts[i], :], y_send.at[0], g_recv.at[i],
            near_a if i < split else near_b,
        )
        for i in range(pieces)
    ]
    y_copies = [
        remote(
            y_out.at[parts[i], :], y_in.at[parts[i], :], y_send.at[0], y_recv.at[i // 4],
            near_b if i < split else near_a,
        )
        for i in range(pieces)
    ]
    for i in order:
        part = parts[i]
        a = att[part, :] + dot(qg[part, :], carried)
        spread = jnp.mean(a * a, axis=-1, keepdims=True)
        gated[0, part, :] = (a * lax.rsqrt(spread + 1e-05) * act[part, :]).astype(BF16)
        g_copies[i].start()
    landed(w, w_sem.at[0])
    pl.when(scans)(lambda: landed(w_near, hand_sem.at[0]))

    for i in order:
        part = parts[i]
        g_copies[i].wait_recv()
        j = i // split
        y_out[part, :] = (
            dot(gated[0, part, :], w[2 - j]) + dot(gated[1, part, :], w_near[1, j])
        ).astype(BF16)
        y_copies[i].start()
    for i in order:
        part = parts[i]
        mine[part, :] = dot(gated[0, part, :], w[0]) + dot(gated[1, part, :], w_near[0, i // split])
    for i in range(2):
        part = slice(i * split * TOKENS, (i + 1) * split * TOKENS)
        landed(y_in.at[part, :], y_recv.at[i])
        out[part, :] = (mine[part, :] + y_in[part, :].astype(F32)).astype(BF16)

    landed(gated, y_send.at[0])

    @pl.when(feeds)
    def _():
        log_copy.wait_send()
        core_copy.wait_send()
        landed(w_near, sum_send.at[0])
        landed(w_near, hand_sem.at[0])

    @pl.when(scans)
    def _():
        landed(sum_in.at[0 : Z - 1], sum_send.at[0])
        landed(tile_out.at[0 : Z - 1], tile_send.at[0])
        landed(enter_out.at[0 : Z - 1], enter_send.at[0])
        pass_copy.wait_send()
        for x in range(rows_x - 1):

            @pl.when(at_x == x)
            def _():
                landed(row_in.at[0 : rows_x - 1 - x], row_send.at[0])
                landed(total_in.at[0 : rows_x - 1 - x], total_send.at[0])


def shards(n_seq, n_head, queries, key_vectors, values, log_gate, out_gate, norm_gain, out_weight):
    length = queries.shape[0]
    width = out_weight.shape[1] // n_head
    blocks = length // SPAN
    pieces = length // TOKENS
    rows_x = n_seq // 2 // Z
    VM = pltpu.VMEM
    dma = pltpu.SemaphoreType.DMA
    tiles = VM((Z, DK // Z, DV), BF16)
    row = VM((1, DK), F32)
    scratch = [
        VM((length, DK), BF16), VM((length, DK), BF16), VM((length, DV), BF16),
        VM((length, DK), BF16), VM((length, DV), BF16), VM((1, DV), F32),
        VM((3, DV, width), BF16), VM((2, 2, DV, width), BF16),
        VM((blocks, SPAN, DK), F32), VM((blocks, DK), F32), VM((length, DK), BF16),
        VM((length, DK), BF16), VM((length, DV), F32), VM((length, DV), F32), VM((DK, DV), F32),
        row, row, VM((DK, DV), F32), VM((DK, DV), BF16), VM((DK, DV), BF16), VM((DK, 128), F32),
        row, VM((Z, 1, DK), F32), row, VM((rows_x, 1, DK), F32),
        VM((128, DK), F32), VM((DK, 128), F32), VM((DK, 128), F32),
        tiles, tiles, VM((DK // Z, DV), BF16), VM((rows_x, DK // Z, DV), BF16),
        VM((DK // Z, DV), F32), tiles, tiles, VM((Z + rows_x, DK // Z, 128), F32), row,
        VM((2, length, DV), BF16), VM((length, width), F32),
        VM((length, width), BF16), VM((length, width), BF16),
        dma((6,)), dma((1,)), dma((1,)), dma((1,)), dma((1,)), dma((1,)),
        dma((1,)), dma((1,)), dma((1,)), dma((1,)), dma((1,)), dma((1,)),
        dma((1,)), dma((1,)), dma((1,)), dma((1,)),
        dma((pieces,)), dma((1,)), dma((pieces // 4,)),
    ]
    return pl.pallas_call(
        functools.partial(kernel, n_seq, n_head),
        out_shape=pltpu.VMEM((length, width), BF16),
        in_specs=[pl.BlockSpec(memory_space=pl.ANY)] * 7,
        out_specs=pl.BlockSpec(memory_space=pltpu.VMEM),
        scratch_shapes=scratch,
        compiler_params=pltpu.CompilerParams(
            collective_id=0, has_side_effects=True, vmem_limit_bytes=56 * 2**20
        ),
        name="gated_layer",
    )(queries, key_vectors, values, log_gate, out_gate, norm_gain.reshape(1, DV), out_weight)


def solution(mesh):
    in_specs = (
        P("seq", "head"),
        P("seq", "head"),
        P("seq", "head"),
        P("seq", "head"),
        P("seq", "head"),
        P("head"),
        P("head", None),
    )
    out_specs = P("seq", "head")
    body = functools.partial(shards, mesh.shape["seq"], mesh.shape["head"])
    return jax.shard_map(body, mesh=mesh, in_specs=in_specs, out_specs=out_specs, check_vma=False)
```

```python
import functools

import jax
import jax.numpy as jnp
from jax import lax
from jax.experimental import pallas as pl
from jax.experimental.pallas import tpu as pltpu
from jax.sharding import PartitionSpec as P

DK = 256
DV = 512
SPAN = 64
TOKENS = 128
Z = 8
EARLY = 3
F32 = jnp.float32
BF16 = jnp.bfloat16
MESH = pl.DeviceIdType.MESH


def dot(a, b, dims=((1,), (0,))):
    return lax.dot_general(a, b, (dims, ((), ())), preferred_element_type=F32)


def kernel(
    n_seq, n_head,
    q_hbm, k_hbm, v_hbm, g_hbm, o_hbm, gain_hbm, w_hbm,
    out,
    q, k, v, g, o, gain, w, w_near,
    run, ends, kd, qg, att, act, state,
    log_out, log_in, own_state, core_out, core_in, decay,
    sum_out, sum_in, row_out, row_in, sums, spans, row_spans,
    tile_out, tile_in, total_out, total_in, ahead, enter_out, enter_in, fac, lead,
    gated, mine, y_out, y_in,
    load_sem, w_sem, hand_sem, log_sem, core_sem, pass_sem,
    sum_send, sum_recv, row_send, row_recv, tile_send, tile_recv,
    total_send, total_recv, enter_send, enter_recv,
    g_recv, y_send, y_recv,
):
    loads = [
        pltpu.make_async_copy(src, dst, load_sem.at[i])
        for i, (src, dst) in enumerate(
            ((g_hbm, g), (k_hbm, k), (v_hbm, v), (q_hbm, q), (o_hbm, o), (gain_hbm, gain))
        )
    ]
    for load in loads[:3]:
        load.start()
    length = q.shape[0]
    blocks = length // SPAN
    pieces = length // TOKENS
    width = w_hbm.shape[1] // n_head
    rows_x = n_seq // 2 // Z
    part_rows = DK // Z
    copies = DV // 128
    seq = lax.axis_index("seq")
    head = lax.axis_index("head")
    core = lax.rem(seq, 2)
    chip = lax.div(seq, 2)
    feeds = core == 0
    scans = core == 1
    at_x = lax.div(chip, Z)
    at_z = lax.rem(chip, Z)
    head_a = head + 1 - 2 * lax.rem(head, 2)
    head_b = n_head - 1 - head
    head_c = n_head - 1 - head_a
    sibling = {"seq": seq + 1 - 2 * core, "head": head}
    near_a = {"seq": seq, "head": head_a}
    near_b = {"seq": seq, "head": head_b}

    def mate(x, z):
        return {"seq": (x * Z + z) * 2 + core, "head": head}

    in_row = [mate(at_x, lax.rem(at_z + dz, Z)) for dz in (4, 3, 5, 2, 6, 1, 7)]
    later = {dx: mate(lax.rem(at_x + dx, rows_x), at_z) for dx in (2, 1, 3)}

    def columns(which):
        return pl.ds(pl.multiple_of(which * width, 128), width)

    def remote(src, dst, send, recv, device):
        return pltpu.make_async_remote_copy(
            src_ref=src, dst_ref=dst, send_sem=send, recv_sem=recv,
            device_id=device, device_id_type=MESH,
        )

    def landed(ref, sem):
        pltpu.make_async_copy(ref, ref, sem).wait()

    barrier = pltpu.get_barrier_semaphore()

    def greet(friends):
        for friend in friends:
            pl.semaphore_signal(barrier, inc=1, device_id=friend, device_id_type=MESH)

    near = [sibling, near_a, near_b]
    greet(near)
    pl.when(scans)(lambda: greet(in_row + list(later.values())))
    w_loads = [
        pltpu.make_async_copy(w_hbm.at[:, columns(which)], w.at[j], w_sem.at[0])
        for j, which in enumerate((head, head_a, head_b))
    ]
    w_copies = [
        remote(w_hbm.at[:, columns(which)], w_near.at[j, i], sum_send.at[0], (sum_recv, tile_recv)[j].at[0], device)
        for which, j, i, device in (
            (head_c, 1, 0, near_a), (head_c, 1, 1, near_b),
            (head_a, 0, 0, near_a), (head_b, 0, 1, near_b),
        )
    ]
    hand_copies = [
        remote(w_near.at[j], w_near.at[j], hand_sem.at[0], hand_sem.at[0], sibling) for j in (1, 0)
    ]
    log_copy = remote(log_out, log_in, log_sem.at[0], log_sem.at[0], sibling)
    core_copy = remote(core_out, core_in, core_sem.at[0], core_sem.at[0], sibling)

    tri = (
        lax.broadcasted_iota(jnp.int32, (SPAN, SPAN), 0)
        >= lax.broadcasted_iota(jnp.int32, (SPAN, SPAN), 1)
    )
    ones = jnp.where(tri, 1.0, 0.0).astype(BF16)
    loads[0].wait()
    total = jnp.zeros((1, DK), F32)
    endings = []
    for b in range(blocks):
        r = dot(ones, g[b * SPAN : (b + 1) * SPAN, :])
        run[b] = r
        endings.append(r[SPAN - 1 : SPAN, :])
        ends[b : b + 1, :] = total
        total = total + endings[b]
    log_out[...] = total
    loads[1].wait()
    tail = jnp.zeros((1, DK), F32)
    for b in reversed(range(blocks)):
        part = slice(b * SPAN, (b + 1) * SPAN)
        kd[part, :] = (k[part, :].astype(F32) * jnp.exp((endings[b] - run[b]) + tail)).astype(BF16)
        tail = tail + endings[b]
    loads[2].wait()

    @pl.when(feeds)
    def _():
        pl.semaphore_wait(barrier, len(near))
        log_copy.start()

    grown = dot(kd[...], v[...], ((0,), (0,)))

    @pl.when(feeds)
    def _():
        core_out[...] = grown.astype(BF16)
        core_copy.start()

    @pl.when(scans)
    def _():
        own_state[...] = grown

    for load in loads[3:] + w_loads:
        load.start()

    @pl.when(feeds)
    def _():
        for copy in w_copies:
            copy.start()

    def lanes(row):
        return jnp.broadcast_to(row, (128, DK)).T

    def wide(columns):
        return jnp.concatenate([columns] * copies, axis=1)

    def part_of(z):
        return slice(z * part_rows, (z + 1) * part_rows)

    sum_copies = [
        remote(sum_out, sum_in.at[at_z], sum_send.at[0], sum_recv.at[0], device)
        for device in in_row
    ]
    far_first = [lax.rem(at_z + dz, Z) for dz in (4, 3, 5, 2, 6, 1, 7)]
    tile_copies = [
        remote(tile_out.at[z], tile_in.at[at_z], tile_send.at[0], tile_recv.at[0], mate(at_x, z))
        for z in far_first
    ]
    row_copies = {
        dx: remote(row_out, row_in.at[at_x], row_send.at[0], row_recv.at[0], device)
        for dx, device in later.items()
    }
    total_copies = {
        dx: remote(total_out, total_in.at[at_x], total_send.at[0], total_recv.at[0], device)
        for dx, device in later.items()
    }
    enter_copies = [
        remote(enter_out.at[z], enter_in.at[at_z], enter_send.at[0], enter_recv.at[0], mate(at_x, z))
        for z in list(range(EARLY)) + far_first
    ]
    pass_copy = remote(enter_in, enter_in, pass_sem.at[0], pass_sem.at[0], sibling)

    @pl.when(scans)
    def _():
        log_copy.wait_recv()
        sum_out[...] = log_out[...] + log_in[...]
        pl.semaphore_wait(barrier, len(near) + len(in_row) + len(later))
        for copy in sum_copies:
            copy.start()
        decay[...] = lanes(jnp.exp(log_out[...]))
        sum_in[at_z] = sum_out[...]
        core_copy.wait_recv()
        for z in range(Z):
            part = part_of(z)
            tile_out[z] = (
                wide(decay[part, :]) * core_in[part, :].astype(F32) + own_state[part, :]
            ).astype(BF16)
        for copy in tile_copies:
            copy.start()
        tile_in[at_z] = tile_out[at_z]

    for load in loads[3:]:
        load.wait()

    @pl.when(feeds)
    def _():
        state[...] = jnp.zeros_like(state)
        lead[...] = jnp.zeros_like(lead)

    @pl.when(scans)
    def _():
        state[...] = core_in[...].astype(F32)
        lead[...] = log_in[...]


    def local(b, _):
        part = pl.ds(pl.multiple_of(b * SPAN, SPAN), SPAN)
        r = run[b]
        middle = r[SPAN // 2 : SPAN // 2 + 1, :]
        ending = r[SPAN - 1 : SPAN, :]
        before = ends[pl.ds(b, 1), :] + lead[...]
        qf = q[part, :].astype(F32)
        kf = k[part, :].astype(F32)
        qi = qf * jnp.exp(r)
        qg[part, :] = (qi * jnp.exp(before)).astype(BF16)
        q_intra = (qf * jnp.exp(r - middle)).astype(BF16)
        k_intra = (kf * jnp.exp(middle - r)).astype(BF16)
        k_state = (kf * jnp.exp(ending - r)).astype(BF16)
        vb = v[part, :]
        scores = dot(q_intra, k_intra, ((1,), (1,)))
        weights = jnp.where(tri, scores, 0.0).astype(BF16)
        held = state[...]
        att[part, :] = dot(weights, vb) + dot(qi.astype(BF16), held.astype(BF16))
        state[...] = held * wide(lanes(jnp.exp(ending))) + dot(k_state, vb, ((0,), (0,)))
        of = o[part, :].astype(F32)
        act[part, :] = of / (1.0 + jnp.exp(-of)) * gain[...]
        return 0

    lax.fori_loop(0, blocks, local, 0)

    @pl.when(scans)
    def _():
        sums[...] = jnp.zeros_like(sums)
        landed(sum_in.at[0 : Z - 1], sum_recv.at[0])
        along = jnp.zeros((1, DK), F32)
        for z in range(Z):
            sums[z : z + 1, :] = sum_in[z]
            along = along + sum_in[z]
        row_out[...] = along
        for dx, copy in row_copies.items():
            pl.when(at_x + dx < rows_x)(copy.start)
        spans[...] = jnp.exp(sums[...].T)
        own_rows = pl.ds(pl.multiple_of(at_z * part_rows, part_rows), part_rows)

        def spread(table, i):
            fac[i] = jnp.broadcast_to(table[own_rows, :][:, i : i + 1], (part_rows, 128))

        for z in range(Z):
            spread(spans, z)
        landed(tile_in.at[0 : Z - 1], tile_recv.at[0])
        grown = tile_in[0].astype(F32)
        for z in range(1, Z):
            grown = wide(fac[z]) * grown + tile_in[z].astype(F32)
        total_out[...] = grown.astype(BF16)
        for dx, copy in total_copies.items():
            pl.when(at_x + dx < rows_x)(copy.start)
        ahead[...] = jnp.zeros_like(ahead)
        for x in range(1, rows_x):

            @pl.when(at_x == x)
            def _():
                landed(row_in.at[0:x], row_recv.at[0])
                for i in range(x):
                    sums[Z + i : Z + i + 1, :] = row_in[i]
                row_spans[...] = jnp.exp(sums[...].T)
                for i in range(1, x):
                    spread(row_spans, Z + i)
                landed(total_in.at[0:x], total_recv.at[0])
                gone = total_in[0].astype(F32)
                for i in range(1, x):
                    gone = wide(fac[Z + i]) * gone + total_in[i].astype(F32)
                ahead[...] = gone

        entry = ahead[...]
        for z in range(Z):
            enter_out[z] = entry.astype(BF16)
            if z < EARLY:
                pl.when(at_z != z)(enter_copies[z].start)
            if z < Z - 1:
                entry = wide(fac[z]) * entry + tile_in[z].astype(F32)
        for z, copy in zip(far_first, enter_copies[EARLY:]):
            pl.when(z >= EARLY)(copy.start)
        enter_in[at_z] = enter_out[at_z]
        landed(enter_in.at[0 : Z - 1], enter_recv.at[0])
        pass_copy.start()

    @pl.when(feeds)
    def _():
        for j, hand in zip((1, 0), hand_copies):
            landed(w_near.at[j], (sum_recv, tile_recv)[j].at[0])
            hand.start()
        pass_copy.wait_recv()

    carried = enter_in[...].reshape(DK, DV)

    split = pieces // 2
    order = [i + j * split for i in range(split) for j in range(2)]
    parts = [slice(i * TOKENS, (i + 1) * TOKENS) for i in range(pieces)]
    g_copies = [
        remote(
            gated.at[0, parts[i], :], gated.at[1, parts[i], :], y_send.at[0], g_recv.at[i],
            near_a if i < split else near_b,
        )
        for i in range(pieces)
    ]
    y_copies = [
        remote(
            y_out.at[parts[i], :], y_in.at[parts[i], :], y_send.at[0], y_recv.at[i // split],
            near_b if i < split else near_a,
        )
        for i in range(pieces)
    ]
    for i in order:
        part = parts[i]
        a = att[part, :] + dot(qg[part, :], carried)
        spread = jnp.mean(a * a, axis=-1, keepdims=True)
        gated[0, part, :] = (a * lax.rsqrt(spread + 1e-05) * act[part, :]).astype(BF16)
        g_copies[i].start()
    landed(w, w_sem.at[0])
    pl.when(scans)(lambda: landed(w_near, hand_sem.at[0]))

    for i in order:
        part = parts[i]
        g_copies[i].wait_recv()
        j = i // split
        y_out[part, :] = (
            dot(gated[0, part, :], w[2 - j]) + dot(gated[1, part, :], w_near[1, j])
        ).astype(BF16)
        y_copies[i].start()
    for i in order:
        part = parts[i]
        mine[part, :] = dot(gated[0, part, :], w[0]) + dot(gated[1, part, :], w_near[0, i // split])
    for i in range(2):
        part = slice(i * split * TOKENS, (i + 1) * split * TOKENS)
        landed(y_in.at[part, :], y_recv.at[i])
        out[part, :] = (mine[part, :] + y_in[part, :].astype(F32)).astype(BF16)

    landed(gated, y_send.at[0])

    @pl.when(feeds)
    def _():
        log_copy.wait_send()
        core_copy.wait_send()
        landed(w_near, sum_send.at[0])
        landed(w_near, hand_sem.at[0])

    @pl.when(scans)
    def _():
        landed(sum_in.at[0 : Z - 1], sum_send.at[0])
        landed(tile_out.at[0 : Z - 1], tile_send.at[0])
        landed(enter_out.at[0 : Z - 1], enter_send.at[0])
        pass_copy.wait_send()
        for x in range(rows_x - 1):

            @pl.when(at_x == x)
            def _():
                landed(row_in.at[0 : rows_x - 1 - x], row_send.at[0])
                landed(total_in.at[0 : rows_x - 1 - x], total_send.at[0])


def shards(n_seq, n_head, queries, key_vectors, values, log_gate, out_gate, norm_gain, out_weight):
    length = queries.shape[0]
    width = out_weight.shape[1] // n_head
    blocks = length // SPAN
    pieces = length // TOKENS
    rows_x = n_seq // 2 // Z
    VM = pltpu.VMEM
    dma = pltpu.SemaphoreType.DMA
    tiles = VM((Z, DK // Z, DV), BF16)
    row = VM((1, DK), F32)
    scratch = [
        VM((length, DK), BF16), VM((length, DK), BF16), VM((length, DV), BF16),
        VM((length, DK), BF16), VM((length, DV), BF16), VM((1, DV), F32),
        VM((3, DV, width), BF16), VM((2, 2, DV, width), BF16),
        VM((blocks, SPAN, DK), F32), VM((blocks, DK), F32), VM((length, DK), BF16),
        VM((length, DK), BF16), VM((length, DV), F32), VM((length, DV), F32), VM((DK, DV), F32),
        row, row, VM((DK, DV), F32), VM((DK, DV), BF16), VM((DK, DV), BF16), VM((DK, 128), F32),
        row, VM((Z, 1, DK), F32), row, VM((rows_x, 1, DK), F32),
        VM((128, DK), F32), VM((DK, 128), F32), VM((DK, 128), F32),
        tiles, tiles, VM((DK // Z, DV), BF16), VM((rows_x, DK // Z, DV), BF16),
        VM((DK // Z, DV), F32), tiles, tiles, VM((Z + rows_x, DK // Z, 128), F32), row,
        VM((2, length, DV), BF16), VM((length, width), F32),
        VM((length, width), BF16), VM((length, width), BF16),
        dma((6,)), dma((1,)), dma((1,)), dma((1,)), dma((1,)), dma((1,)),
        dma((1,)), dma((1,)), dma((1,)), dma((1,)), dma((1,)), dma((1,)),
        dma((1,)), dma((1,)), dma((1,)), dma((1,)),
        dma((pieces,)), dma((1,)), dma((2,)),
    ]
    return pl.pallas_call(
        functools.partial(kernel, n_seq, n_head),
        out_shape=pltpu.VMEM((length, width), BF16),
        in_specs=[pl.BlockSpec(memory_space=pl.ANY)] * 7,
        out_specs=pl.BlockSpec(memory_space=pltpu.VMEM),
        scratch_shapes=scratch,
        compiler_params=pltpu.CompilerParams(
            collective_id=0, has_side_effects=True, vmem_limit_bytes=56 * 2**20
        ),
        name="gated_layer",
    )(queries, key_vectors, values, log_gate, out_gate, norm_gain.reshape(1, DV), out_weight)


def solution(mesh):
    in_specs = (
        P("seq", "head"),
        P("seq", "head"),
        P("seq", "head"),
        P("seq", "head"),
        P("seq", "head"),
        P("head"),
        P("head", None),
    )
    out_specs = P("seq", "head")
    body = functools.partial(shards, mesh.shape["seq"], mesh.shape["head"])
    return jax.shard_map(body, mesh=mesh, in_specs=in_specs, out_specs=out_specs, check_vma=False)
```

```python
import functools

import jax
import jax.numpy as jnp
from jax import lax
from jax.experimental import pallas as pl
from jax.experimental.pallas import tpu as pltpu
from jax.sharding import PartitionSpec as P

DK = 256
DV = 512
SPAN = 64
TOKENS = 64
Z = 8
EARLY = 3
F32 = jnp.float32
BF16 = jnp.bfloat16
MESH = pl.DeviceIdType.MESH


def dot(a, b, dims=((1,), (0,))):
    return lax.dot_general(a, b, (dims, ((), ())), preferred_element_type=F32)


def kernel(
    n_seq, n_head,
    q_hbm, k_hbm, v_hbm, g_hbm, o_hbm, gain_hbm, w_hbm,
    out,
    q, k, v, g, o, gain, w, w_near,
    run, ends, kd, qg, att, act, state,
    log_out, log_in, own_state, core_out, core_in, decay,
    sum_out, sum_in, row_out, row_in, sums, spans, row_spans,
    tile_out, tile_in, total_out, total_in, ahead, enter_out, enter_in, fac, lead,
    gated, mine, y_out, y_in,
    load_sem, w_sem, hand_sem, log_sem, core_sem, pass_sem,
    sum_send, sum_recv, row_send, row_recv, tile_send, tile_recv,
    total_send, total_recv, enter_send, enter_recv,
    g_recv, y_send, y_recv,
):
    loads = [
        pltpu.make_async_copy(src, dst, load_sem.at[i])
        for i, (src, dst) in enumerate(
            ((g_hbm, g), (k_hbm, k), (v_hbm, v), (q_hbm, q), (o_hbm, o), (gain_hbm, gain))
        )
    ]
    for load in loads[:3]:
        load.start()
    length = q.shape[0]
    blocks = length // SPAN
    pieces = length // TOKENS
    width = w_hbm.shape[1] // n_head
    rows_x = n_seq // 2 // Z
    part_rows = DK // Z
    copies = DV // 128
    seq = lax.axis_index("seq")
    head = lax.axis_index("head")
    core = lax.rem(seq, 2)
    chip = lax.div(seq, 2)
    feeds = core == 0
    scans = core == 1
    at_x = lax.div(chip, Z)
    at_z = lax.rem(chip, Z)
    head_a = head + 1 - 2 * lax.rem(head, 2)
    head_b = n_head - 1 - head
    head_c = n_head - 1 - head_a
    sibling = {"seq": seq + 1 - 2 * core, "head": head}
    near_a = {"seq": seq, "head": head_a}
    near_b = {"seq": seq, "head": head_b}

    def mate(x, z):
        return {"seq": (x * Z + z) * 2 + core, "head": head}

    in_row = [mate(at_x, lax.rem(at_z + dz, Z)) for dz in (4, 3, 5, 2, 6, 1, 7)]
    later = {dx: mate(lax.rem(at_x + dx, rows_x), at_z) for dx in (2, 1, 3)}

    def columns(which):
        return pl.ds(pl.multiple_of(which * width, 128), width)

    def remote(src, dst, send, recv, device):
        return pltpu.make_async_remote_copy(
            src_ref=src, dst_ref=dst, send_sem=send, recv_sem=recv,
            device_id=device, device_id_type=MESH,
        )

    def landed(ref, sem):
        pltpu.make_async_copy(ref, ref, sem).wait()

    barrier = pltpu.get_barrier_semaphore()

    def greet(friends):
        for friend in friends:
            pl.semaphore_signal(barrier, inc=1, device_id=friend, device_id_type=MESH)

    near = [sibling, near_a, near_b]
    greet(near)
    pl.when(scans)(lambda: greet(in_row + list(later.values())))
    w_loads = [
        pltpu.make_async_copy(w_hbm.at[:, columns(which)], w.at[j], w_sem.at[0])
        for j, which in enumerate((head, head_a, head_b))
    ]
    w_copies = [
        remote(w_hbm.at[:, columns(which)], w_near.at[j, i], sum_send.at[0], (sum_recv, tile_recv)[j].at[0], device)
        for which, j, i, device in (
            (head_c, 1, 0, near_a), (head_c, 1, 1, near_b),
            (head_a, 0, 0, near_a), (head_b, 0, 1, near_b),
        )
    ]
    hand_copies = [
        remote(w_near.at[j], w_near.at[j], hand_sem.at[0], hand_sem.at[0], sibling) for j in (1, 0)
    ]
    log_copy = remote(log_out, log_in, log_sem.at[0], log_sem.at[0], sibling)
    core_copy = remote(core_out, core_in, core_sem.at[0], core_sem.at[0], sibling)

    tri = (
        lax.broadcasted_iota(jnp.int32, (SPAN, SPAN), 0)
        >= lax.broadcasted_iota(jnp.int32, (SPAN, SPAN), 1)
    )
    ones = jnp.where(tri, 1.0, 0.0).astype(BF16)
    loads[0].wait()
    total = jnp.zeros((1, DK), F32)
    endings = []
    for b in range(blocks):
        r = dot(ones, g[b * SPAN : (b + 1) * SPAN, :])
        run[b] = r
        endings.append(r[SPAN - 1 : SPAN, :])
        ends[b : b + 1, :] = total
        total = total + endings[b]
    log_out[...] = total

    @pl.when(feeds)
    def _():
        pl.semaphore_wait(barrier, len(near))
        log_copy.start()

    loads[1].wait()
    tail = jnp.zeros((1, DK), F32)
    for b in reversed(range(blocks)):
        part = slice(b * SPAN, (b + 1) * SPAN)
        kd[part, :] = (k[part, :].astype(F32) * jnp.exp((endings[b] - run[b]) + tail)).astype(BF16)
        tail = tail + endings[b]
    loads[2].wait()

    grown = dot(kd[...], v[...], ((0,), (0,)))

    @pl.when(feeds)
    def _():
        core_out[...] = grown.astype(BF16)
        core_copy.start()

    @pl.when(scans)
    def _():
        own_state[...] = grown

    for load in loads[3:] + w_loads:
        load.start()

    @pl.when(feeds)
    def _():
        for copy in w_copies:
            copy.start()

    def lanes(row):
        return jnp.broadcast_to(row, (128, DK)).T

    def wide(columns):
        return jnp.concatenate([columns] * copies, axis=1)

    def part_of(z):
        return slice(z * part_rows, (z + 1) * part_rows)

    sum_copies = [
        remote(sum_out, sum_in.at[at_z], sum_send.at[0], sum_recv.at[0], device)
        for device in in_row
    ]
    far_first = [lax.rem(at_z + dz, Z) for dz in (4, 3, 5, 2, 6, 1, 7)]
    tile_copies = [
        remote(tile_out.at[z], tile_in.at[at_z], tile_send.at[0], tile_recv.at[0], mate(at_x, z))
        for z in far_first
    ]
    row_copies = {
        dx: remote(row_out, row_in.at[at_x], row_send.at[0], row_recv.at[0], device)
        for dx, device in later.items()
    }
    total_copies = {
        dx: remote(total_out, total_in.at[at_x], total_send.at[0], total_recv.at[0], device)
        for dx, device in later.items()
    }
    enter_copies = [
        remote(enter_out.at[z], enter_in.at[at_z], enter_send.at[0], enter_recv.at[0], mate(at_x, z))
        for z in list(range(EARLY)) + far_first
    ]
    pass_copy = remote(enter_in, enter_in, pass_sem.at[0], pass_sem.at[0], sibling)

    @pl.when(scans)
    def _():
        log_copy.wait_recv()
        sum_out[...] = log_out[...] + log_in[...]
        pl.semaphore_wait(barrier, len(near) + len(in_row) + len(later))
        for copy in sum_copies:
            copy.start()
        decay[...] = lanes(jnp.exp(log_out[...]))
        sum_in[at_z] = sum_out[...]
        core_copy.wait_recv()
        for z in range(Z):
            part = part_of(z)
            tile_out[z] = (
                wide(decay[part, :]) * core_in[part, :].astype(F32) + own_state[part, :]
            ).astype(BF16)
        for copy in tile_copies:
            copy.start()
        tile_in[at_z] = tile_out[at_z]

    for load in loads[3:]:
        load.wait()

    @pl.when(feeds)
    def _():
        state[...] = jnp.zeros_like(state)
        lead[...] = jnp.zeros_like(lead)

    @pl.when(scans)
    def _():
        state[...] = core_in[...].astype(F32)
        lead[...] = log_in[...]


    def local(b, _):
        part = pl.ds(pl.multiple_of(b * SPAN, SPAN), SPAN)
        r = run[b]
        middle = r[SPAN // 2 : SPAN // 2 + 1, :]
        ending = r[SPAN - 1 : SPAN, :]
        before = ends[pl.ds(b, 1), :] + lead[...]
        qf = q[part, :].astype(F32)
        kf = k[part, :].astype(F32)
        qi = qf * jnp.exp(r)
        qg[part, :] = (qi * jnp.exp(before)).astype(BF16)
        q_intra = (qf * jnp.exp(r - middle)).astype(BF16)
        k_intra = (kf * jnp.exp(middle - r)).astype(BF16)
        k_state = (kf * jnp.exp(ending - r)).astype(BF16)
        vb = v[part, :]
        scores = dot(q_intra, k_intra, ((1,), (1,)))
        weights = jnp.where(tri, scores, 0.0).astype(BF16)
        held = state[...]
        att[part, :] = dot(weights, vb) + dot(qi.astype(BF16), held.astype(BF16))
        state[...] = held * wide(lanes(jnp.exp(ending))) + dot(k_state, vb, ((0,), (0,)))
        of = o[part, :].astype(F32)
        act[part, :] = of / (1.0 + jnp.exp(-of)) * gain[...]
        return 0

    lax.fori_loop(0, blocks, local, 0)

    @pl.when(scans)
    def _():
        sums[...] = jnp.zeros_like(sums)
        landed(sum_in.at[0 : Z - 1], sum_recv.at[0])
        along = jnp.zeros((1, DK), F32)
        for z in range(Z):
            sums[z : z + 1, :] = sum_in[z]
            along = along + sum_in[z]
        row_out[...] = along
        for dx, copy in row_copies.items():
            pl.when(at_x + dx < rows_x)(copy.start)
        spans[...] = jnp.exp(sums[...].T)
        own_rows = pl.ds(pl.multiple_of(at_z * part_rows, part_rows), part_rows)

        def spread(table, i):
            fac[i] = jnp.broadcast_to(table[own_rows, :][:, i : i + 1], (part_rows, 128))

        for z in range(Z):
            spread(spans, z)
        landed(tile_in.at[0 : Z - 1], tile_recv.at[0])
        grown = tile_in[0].astype(F32)
        for z in range(1, Z):
            grown = wide(fac[z]) * grown + tile_in[z].astype(F32)
        total_out[...] = grown.astype(BF16)
        for dx, copy in total_copies.items():
            pl.when(at_x + dx < rows_x)(copy.start)
        ahead[...] = jnp.zeros_like(ahead)
        for x in range(1, rows_x):

            @pl.when(at_x == x)
            def _():
                landed(row_in.at[0:x], row_recv.at[0])
                for i in range(x):
                    sums[Z + i : Z + i + 1, :] = row_in[i]
                row_spans[...] = jnp.exp(sums[...].T)
                for i in range(1, x):
                    spread(row_spans, Z + i)
                landed(total_in.at[0:x], total_recv.at[0])
                gone = total_in[0].astype(F32)
                for i in range(1, x):
                    gone = wide(fac[Z + i]) * gone + total_in[i].astype(F32)
                ahead[...] = gone

        entry = ahead[...]
        for z in range(Z):
            enter_out[z] = entry.astype(BF16)
            if z < EARLY:
                pl.when(at_z != z)(enter_copies[z].start)
            if z < Z - 1:
                entry = wide(fac[z]) * entry + tile_in[z].astype(F32)
        for z, copy in zip(far_first, enter_copies[EARLY:]):
            pl.when(z >= EARLY)(copy.start)
        enter_in[at_z] = enter_out[at_z]
        landed(enter_in.at[0 : Z - 1], enter_recv.at[0])
        pass_copy.start()

    @pl.when(feeds)
    def _():
        for j, hand in zip((1, 0), hand_copies):
            landed(w_near.at[j], (sum_recv, tile_recv)[j].at[0])
            hand.start()
        pass_copy.wait_recv()

    carried = enter_in[...].reshape(DK, DV)

    split = pieces // 2
    order = [i + j * split for i in range(split) for j in range(2)]
    parts = [slice(i * TOKENS, (i + 1) * TOKENS) for i in range(pieces)]
    g_copies = [
        remote(
            gated.at[0, parts[i], :], gated.at[1, parts[i], :], y_send.at[0], g_recv.at[i],
            near_a if i < split else near_b,
        )
        for i in range(pieces)
    ]
    y_copies = [
        remote(
            y_out.at[parts[i], :], y_in.at[parts[i], :], y_send.at[0], y_recv.at[i // 4],
            near_b if i < split else near_a,
        )
        for i in range(pieces)
    ]
    for i in order:
        part = parts[i]
        a = att[part, :] + dot(qg[part, :], carried)
        spread = jnp.mean(a * a, axis=-1, keepdims=True)
        gated[0, part, :] = (a * lax.rsqrt(spread + 1e-05) * act[part, :]).astype(BF16)
        g_copies[i].start()
    landed(w, w_sem.at[0])
    pl.when(scans)(lambda: landed(w_near, hand_sem.at[0]))

    for i in order:
        part = parts[i]
        g_copies[i].wait_recv()
        j = i // split
        y_out[part, :] = (
            dot(gated[0, part, :], w[2 - j]) + dot(gated[1, part, :], w_near[1, j])
        ).astype(BF16)
        y_copies[i].start()
    for i in order:
        part = parts[i]
        mine[part, :] = dot(gated[0, part, :], w[0]) + dot(gated[1, part, :], w_near[0, i // split])
    for i in range(2):
        part = slice(i * split * TOKENS, (i + 1) * split * TOKENS)
        landed(y_in.at[part, :], y_recv.at[i])
        out[part, :] = (mine[part, :] + y_in[part, :].astype(F32)).astype(BF16)

    landed(gated, y_send.at[0])

    @pl.when(feeds)
    def _():
        log_copy.wait_send()
        core_copy.wait_send()
        landed(w_near, sum_send.at[0])
        landed(w_near, hand_sem.at[0])

    @pl.when(scans)
    def _():
        landed(sum_in.at[0 : Z - 1], sum_send.at[0])
        landed(tile_out.at[0 : Z - 1], tile_send.at[0])
        landed(enter_out.at[0 : Z - 1], enter_send.at[0])
        pass_copy.wait_send()
        for x in range(rows_x - 1):

            @pl.when(at_x == x)
            def _():
                landed(row_in.at[0 : rows_x - 1 - x], row_send.at[0])
                landed(total_in.at[0 : rows_x - 1 - x], total_send.at[0])


def shards(n_seq, n_head, queries, key_vectors, values, log_gate, out_gate, norm_gain, out_weight):
    length = queries.shape[0]
    width = out_weight.shape[1] // n_head
    blocks = length // SPAN
    pieces = length // TOKENS
    rows_x = n_seq // 2 // Z
    VM = pltpu.VMEM
    dma = pltpu.SemaphoreType.DMA
    tiles = VM((Z, DK // Z, DV), BF16)
    row = VM((1, DK), F32)
    scratch = [
        VM((length, DK), BF16), VM((length, DK), BF16), VM((length, DV), BF16),
        VM((length, DK), BF16), VM((length, DV), BF16), VM((1, DV), F32),
        VM((3, DV, width), BF16), VM((2, 2, DV, width), BF16),
        VM((blocks, SPAN, DK), F32), VM((blocks, DK), F32), VM((length, DK), BF16),
        VM((length, DK), BF16), VM((length, DV), F32), VM((length, DV), F32), VM((DK, DV), F32),
        row, row, VM((DK, DV), F32), VM((DK, DV), BF16), VM((DK, DV), BF16), VM((DK, 128), F32),
        row, VM((Z, 1, DK), F32), row, VM((rows_x, 1, DK), F32),
        VM((128, DK), F32), VM((DK, 128), F32), VM((DK, 128), F32),
        tiles, tiles, VM((DK // Z, DV), BF16), VM((rows_x, DK // Z, DV), BF16),
        VM((DK // Z, DV), F32), tiles, tiles, VM((Z + rows_x, DK // Z, 128), F32), row,
        VM((2, length, DV), BF16), VM((length, width), F32),
        VM((length, width), BF16), VM((length, width), BF16),
        dma((6,)), dma((1,)), dma((1,)), dma((1,)), dma((1,)), dma((1,)),
        dma((1,)), dma((1,)), dma((1,)), dma((1,)), dma((1,)), dma((1,)),
        dma((1,)), dma((1,)), dma((1,)), dma((1,)),
        dma((pieces,)), dma((1,)), dma((pieces // 4,)),
    ]
    return pl.pallas_call(
        functools.partial(kernel, n_seq, n_head),
        out_shape=pltpu.VMEM((length, width), BF16),
        in_specs=[pl.BlockSpec(memory_space=pl.ANY)] * 7,
        out_specs=pl.BlockSpec(memory_space=pltpu.VMEM),
        scratch_shapes=scratch,
        compiler_params=pltpu.CompilerParams(
            collective_id=0, has_side_effects=True, vmem_limit_bytes=56 * 2**20
        ),
        name="gated_layer",
    )(queries, key_vectors, values, log_gate, out_gate, norm_gain.reshape(1, DV), out_weight)


def solution(mesh):
    in_specs = (
        P("seq", "head"),
        P("seq", "head"),
        P("seq", "head"),
        P("seq", "head"),
        P("seq", "head"),
        P("head"),
        P("head", None),
    )
    out_specs = P("seq", "head")
    body = functools.partial(shards, mesh.shape["seq"], mesh.shape["head"])
    return jax.shard_map(body, mesh=mesh, in_specs=in_specs, out_specs=out_specs, check_vma=False)
```
